256 devices in a mesh: row: 16 (over z, core), col: 16 (over y, x).
Axes of the slice: x: 4, y: 4, z: 8, core: 2. Of those that a mesh axis runs over, the one named last changes fastest.
Arguments:
- act_codes: int32 [2048, 7168], P('col', 'row'), may hold values from -127 to 127
- act_scales: float32 [2048, 112], P('col', 'row'), may hold values from 0.005 to 0.03
- gate_weight: bfloat16 [7168, 18432], P('row', 'col'), may hold values from -0.0625 to 0.0625
- up_weight: bfloat16 [7168, 18432], P('row', 'col'), may hold values from -0.0625 to 0.0625
- down_weight: bfloat16 [18432, 7168], P('col', 'row'), may hold values from -0.046875 to 0.046875
Outputs:
- mixed: bfloat16 [2048, 7168], P('col', 'row')
The draws below stay inside these ranges and needn't reach their ends.
All inputs are finite; a program needn't handle non-finite values.
Results may differ from the reference program's by a relative error of at most 0.03.
Values may be sent and summed in bfloat16 or wider, within the bound.
A program may use at most 128 MiB of HBM per device.

```python
import math
import jax
import jax.numpy as jnp
from jax import lax

D = 7168
FF = 18432
QB = 64
TOKENS = 2048
D_ROW = 448
FF_COL = 1152
BLOCKS = 112
N_ROW = 16
N_COL = 16


def place_ends(entries, rng, least, top_value):
    index_at = [jax.random.randint(jax.random.fold_in(rng, axis), (), 0, length) for axis, length in enumerate(entries.shape)]
    widest = entries.shape.index(max(entries.shape))
    next_to = index_at[:widest] + [(index_at[widest] + 1) % entries.shape[widest]] + index_at[widest + 1:]
    return entries.at[tuple(index_at)].set(least).at[tuple(next_to)].set(top_value)


def shard_levels(own_key, dims, cuts, smallest, high):
    loudness, own = 1.0, jax.random.fold_in(own_key, 6)
    for axis_at, blocks in cuts:
        steps = jnp.exp(jax.random.uniform(jax.random.fold_in(own, axis_at), (blocks,), jnp.float32, smallest / len(cuts), high / len(cuts)))
        loudness = loudness * jnp.repeat(steps, dims[axis_at] // blocks).reshape([-1 if axis == axis_at else 1 for axis in range(len(dims))])
    return loudness


def centred(key, extent, width, most, cuts=(), kind=jnp.bfloat16):
    values = jax.random.normal(key, extent, jnp.float32) * width
    if len(cuts) > 0:
        values = shard_levels(key, extent, cuts, -0.22, 0.18) * values
    return jnp.clip(values, min=-most, max=most).astype(kind)


def setup_inputs(seed: int = 0) -> dict:
    keys = jax.random.split(jax.random.key(seed), 6)
    act_codes = place_ends(jax.random.randint(keys[0], (TOKENS, D), -127, 128), jax.random.fold_in(keys[0], 1), -127, 127).astype(jnp.int32)
    act_scales = jnp.clip(jnp.exp(math.log(0.03) - 1.7917595 * jax.random.uniform(keys[1], (TOKENS, BLOCKS), jnp.float32) ** shard_levels(keys[1], (TOKENS, BLOCKS), ((0, 16), (1, 16)), -0.2, 0.2)), 0.005, 0.03)
    gate_weight = centred(keys[2], (D, FF), D ** -0.5, 0.0625, ((0, 16), (1, 16)))
    up_weight = centred(keys[3], (D, FF), D ** -0.5, 0.0625, ((0, 16), (1, 16)))
    down_weight = centred(keys[4], (FF, D), FF ** -0.5, 0.046875, ((0, 16), (1, 16)))
    return dict(act_codes=act_codes, act_scales=act_scales, gate_weight=gate_weight, up_weight=up_weight, down_weight=down_weight)


def dequantize(act_codes, act_scales):
    rows = act_codes.shape[0]
    blocked = act_codes.astype(jnp.float32).reshape(rows, BLOCKS, QB)
    scaled = blocked * act_scales[:, :, None]
    return scaled.reshape(rows, D).astype(jnp.bfloat16)


def rounded(value):
    narrow = lax.optimization_barrier(value.astype(jnp.bfloat16))
    return narrow.astype(jnp.float32)


def reference(act_codes, act_scales, gate_weight, up_weight, down_weight):
    acts = dequantize(act_codes, act_scales)

    def feature_group(index, totals):
        start = (index * D_ROW).astype(jnp.int32)
        slab = lax.dynamic_slice_in_dim(acts, start, D_ROW, 1)
        gate_rows = lax.dynamic_slice_in_dim(gate_weight, start, D_ROW, 0)
        up_rows = lax.dynamic_slice_in_dim(up_weight, start, D_ROW, 0)
        gate_part = rounded(jnp.dot(slab, gate_rows, preferred_element_type=jnp.float32))
        up_part = rounded(jnp.dot(slab, up_rows, preferred_element_type=jnp.float32))
        return (totals[0] + gate_part, totals[1] + up_part)

    empty = jnp.zeros((TOKENS, FF), jnp.float32)
    gate, up = lax.fori_loop(0, N_ROW, feature_group, (empty, empty))
    hidden = (jax.nn.silu(gate) * up).astype(jnp.bfloat16)

    def hidden_group(index, total):
        start = (index * FF_COL).astype(jnp.int32)
        slab = lax.dynamic_slice_in_dim(hidden, start, FF_COL, 1)
        rows_down = lax.dynamic_slice_in_dim(down_weight, start, FF_COL, 0)
        return total + rounded(jnp.dot(slab, rows_down, preferred_element_type=jnp.float32))

    mixed = lax.fori_loop(0, N_COL, hidden_group, jnp.zeros((TOKENS, D), jnp.float32))
    return mixed.astype(jnp.bfloat16)
```

```python
import functools

import jax
import jax.numpy as jnp
from jax import lax
from jax.experimental import pallas as pl
from jax.experimental.pallas import tpu as pltpu
from jax.sharding import PartitionSpec as P

MESH = pl.DeviceIdType.MESH
F32 = jnp.float32
BF16 = jnp.bfloat16

NZ, NX, NY, CORES = 8, 4, 4, 2
TOK = 128
HALF = TOK // CORES
D_ROW = 448
LOW = 384
D_CHIP = CORES * D_ROW
FF = 1152
GU = 2 * FF
PAD = 512
PIECE = 32
STRIP = 16
QB = 64

GROUPS = (
    ((0, 0), (1, 0), (3, 0), (0, 1)),
    ((0, 3), (1, 1), (2, 0), (0, 2)),
    ((1, 3), (3, 1), (3, 3), (1, 2)),
    ((3, 2), (2, 1), (2, 3), (2, 2)),
)
NQ = len(GROUPS)
SLOT = {s: i for i, s in enumerate(s for g in GROUPS for s in g)}
ROWS = HALF * 4
PASS_ON = {
    (0, 0): ((1, 0), (-1, 0), (0, 1), (0, -1)),
    (1, 0): ((0, 1), (0, -1), (1, 0)),
    (3, 0): ((0, 1), (0, -1)),
    (0, 1): ((0, 1),),
    (1, 1): ((0, 1),),
    (3, 3): ((0, -1),),
    (2, 0): ((0, 1), (0, -1)),
    (2, 3): ((0, -1),),
}
LAST = NZ - 1
HOPS = NZ // 2


def steps_of(part, slot):
    if part == 0:
        return PASS_ON.get(slot, ())
    return tuple((b, a) for a, b in PASS_ON.get((slot[1], slot[0]), ()))


def max_hop(d, q):
    return HOPS if (q + d) % 2 == 0 else HOPS - 1


def order():
    hops = {1: [(1, 0), (3, 0), (0, 1), (0, 3)],
            2: [(2, 0), (0, 2), (1, 1), (3, 1), (1, 3), (3, 3)],
            3: [(1, 2), (2, 1), (3, 2), (2, 3)],
            4: [(2, 2)]}
    ops = []
    for tick in range(LAST + HOPS + NQ):
        if tick < NQ:
            ops += [("acts", s) for s in hops[tick + 1]]
            ops += [("up", tick)]
        for q in reversed(range(NQ)):
            stage = tick - q
            if 0 <= stage <= LAST + HOPS:
                ops.append(("ring", q, stage))
        hop = tick - (NQ - 1) - LAST
        if hop == 0:
            ops.append(("down", 0, 0))
        elif 1 <= hop < HOPS:
            ops += [("down", 2 * hop - 1, NZ - hop), ("down", 2 * hop, hop)]
        elif hop == HOPS:
            ops.append(("down", NZ - 1, HOPS))
    return ops


def kernel(
    codes_hbm, scales_hbm, gate_hbm, up_hbm, down_hbm, out_ref,
    codes, scales, staged, swapped, acts, w, wd, part, ring, hidden, outs, finals,
    in_sem, w_local, w_send, w_recv, swap_sem, a_send, a_recv, r_send, r_recv, h_send, h_recv, f_send, f_recv,
):
    row, col = lax.axis_index("row"), lax.axis_index("col")
    z, core = row // CORES, row % CORES
    y, x = col // NX, col % NX
    other = 1 - core

    def along_z(step):
        return ((z + NZ + step) % NZ * CORES + core, col)

    def in_plane(sx, sy):
        return (row, (y + NY + sy) % NY * NX + (x + NX + sx) % NX)

    partner = (z * CORES + other, col)
    neighbours = (along_z(1), along_z(-1), in_plane(1, 0), in_plane(-1, 0), in_plane(0, 1), in_plane(0, -1))

    def remote(src, dst, send, recv, device):
        return pltpu.make_async_remote_copy(
            src_ref=src, dst_ref=dst, send_sem=send, recv_sem=recv, device_id=device, device_id_type=MESH
        )

    in_codes = pltpu.make_async_copy(codes_hbm, codes, in_sem.at[0])
    in_scales = pltpu.make_async_copy(scales_hbm, scales, in_sem.at[1])
    in_codes.start()
    in_scales.start()

    low = pl.ds(pl.multiple_of(core * LOW, 128), LOW)
    tail = pl.ds(pl.multiple_of(CORES * LOW + core * (D_ROW - LOW), 64), D_ROW - LOW)
    pieces = [
        (gate_hbm.at[pl.ds(0, LOW)], w.at[low, pl.ds(0, FF)]),
        (gate_hbm.at[pl.ds(LOW, D_ROW - LOW)], w.at[tail, pl.ds(0, FF)]),
        (up_hbm.at[pl.ds(0, LOW)], w.at[low, pl.ds(FF, FF)]),
        (up_hbm.at[pl.ds(LOW, D_ROW - LOW)], w.at[tail, pl.ds(FF, FF)]),
        (down_hbm, wd.at[core]),
    ]
    local = [pltpu.make_async_copy(src, dst, w_local.at[i]) for i, (src, dst) in enumerate(pieces)]
    pushed = [remote(src, dst, w_send.at[i], w_recv.at[i], partner) for i, (src, dst) in enumerate(pieces)]
    for copy in local:
        copy.start()

    barrier = pltpu.get_barrier_semaphore()
    for device in (partner, *neighbours):
        pl.semaphore_signal(barrier, inc=1, device_id=device, device_id_type=MESH)

    in_codes.wait()
    in_scales.wait()
    lane = lax.broadcasted_iota(jnp.int32, (TOK, 128), 1)
    for tile in range(D_ROW // 128):
        cut = pl.ds(tile * 128, 128)
        scale = jnp.where(
            lane < QB, scales[:, 2 * tile : 2 * tile + 1], scales[:, 2 * tile + 1 : 2 * tile + 2]
        )
        staged[:, cut] = (codes[:, cut].astype(F32) * scale).astype(BF16)
    last = codes[:, LOW:D_ROW].astype(F32) * scales[:, 6:7]
    staged[:, LOW:PAD] = jnp.concatenate([last, jnp.zeros_like(last)], axis=1).astype(BF16)

    pl.semaphore_wait(barrier, 1 + len(neighbours))
    swap = remote(
        staged.at[pl.ds(pl.multiple_of(other * HALF, HALF), HALF)], swapped, swap_sem.at[0], swap_sem.at[1], partner
    )
    swap.start()
    for copy in pushed:
        copy.start()
    swap.wait_recv()
    mine = staged[pl.ds(pl.multiple_of(core * HALF, HALF), HALF), :].astype(F32)
    theirs = swapped[...].astype(F32)
    first = jnp.where(core == 0, mine, theirs)
    second = jnp.where(core == 0, theirs, mine)
    acts[0:HALF, 0:LOW] = first[:, 0:LOW].astype(BF16)
    acts[0:HALF, LOW : 2 * LOW] = second[:, 0:LOW].astype(BF16)
    acts[0:HALF, 2 * LOW : D_CHIP] = (first[:, LOW:PAD] + pltpu.roll(second[:, LOW:PAD], QB, 1)).astype(BF16)

    def acts_rows(slot, half):
        return acts.at[pl.ds(SLOT[slot] * HALF + half * PIECE, PIECE)]

    def pass_on(slot, half):
        for sx, sy in steps_of(half, slot):
            there = ((slot[0] + sx) % NX, (slot[1] + sy) % NY)
            remote(
                acts_rows(slot, half), acts_rows(there, half), a_send, a_recv.at[half, SLOT[there]], in_plane(sx, sy)
            ).start()

    for half in range(2):
        pass_on((0, 0), half)

    def take_acts(slot):
        for half in range(2):
            rows = acts_rows(slot, half)
            remote(rows, rows, a_send, a_recv.at[half, SLOT[slot]], partner).wait_recv()
            pass_on(slot, half)

    def multiply(q):
        if q == 0:
            for i in range(4):
                local[i].wait()
                pushed[i].wait_recv()

        def tile(n, carry):
            cut = pl.ds(pl.multiple_of(n * 256, 256), 256)
            part[q, :, cut] = jnp.dot(
                acts[q * ROWS : (q + 1) * ROWS, :], w[:, cut], preferred_element_type=F32
            ).astype(BF16)
            return carry

        lax.fori_loop(0, GU // 256, tile, 0)

    def strip(q, d, owner):
        return part.at[q, pl.ds(pl.multiple_of(owner * PIECE + d * STRIP, STRIP), STRIP)]

    def arrived(ref, sem):
        remote(ref, ref, r_send, sem, partner).wait_recv()

    def piece(owner, q):
        return hidden.at[owner, pl.ds(q * PIECE, PIECE)]

    def ring_step(q, stage):
        for d in range(2):
            toward = 1 if d == 0 else -1
            if stage < LAST:
                owner = (z + NZ - toward * (stage + 1)) % NZ
                src = strip(q, d, owner)
                if stage > 0:
                    got = ring.at[d, q, stage - 1]
                    arrived(got, r_recv.at[d, q, stage - 1])
                    got[...] = (got[...].astype(F32) + src[...].astype(F32)).astype(BF16)
                    src = got
                remote(src, ring.at[d, q, stage], r_send, r_recv.at[d, q, stage], along_z(toward)).start()
            elif stage == LAST:
                got = ring.at[d, q, stage - 1]
                arrived(got, r_recv.at[d, q, stage - 1])
                own = strip(q, d, z)
                gate = got[:, 0:FF].astype(F32) + own[:, 0:FF].astype(F32)
                up = got[:, FF:GU].astype(F32) + own[:, FF:GU].astype(F32)
                value = gate / (1.0 + jnp.exp(-gate)) * up
                hidden[z, pl.ds(q * PIECE + d * STRIP, STRIP), :] = value.astype(BF16)
        if stage >= LAST:
            hop = stage - LAST
            for d in range(2):
                toward = 1 if d == 0 else -1
                if hop > max_hop(d, q):
                    continue
                ref = piece((z + NZ - toward * hop) % NZ, q)
                if hop > 0:
                    arrived(ref, h_recv.at[d, q, hop - 1])
                if hop < max_hop(d, q):
                    remote(ref, ref, h_send, h_recv.at[d, q, hop], along_z(toward)).start()

    def lookup(q, k, axis):
        packed = sum(s[axis] * 4**i for i, s in enumerate(GROUPS[q]))
        return packed // ((1 + 3 * (k % 2)) * (1 + 15 * (k // 2))) % 4

    def down(turn, offset):
        if turn == 0:
            local[4].wait()
            pushed[4].wait_recv()
        owner = (z + offset) % NZ
        for e in range(CORES):
            outs[turn, e, :, 0:D_ROW] = jnp.dot(
                hidden[owner], wd[e], preferred_element_type=F32
            ).astype(BF16)
        k = owner // 2
        to_rows = pl.ds(pl.multiple_of(core * HALF + owner % 2 * PIECE, PIECE), PIECE)
        for q in range(NQ):
            there = (y + NY - lookup(q, k, 1)) % NY * NX + (x + NX - lookup(q, k, 0)) % NX
            from_rows = pl.ds(q * PIECE, PIECE)

            def send(to_core, sem):
                remote(
                    outs.at[turn, to_core, from_rows],
                    finals.at[q * 4 + k, to_rows],
                    f_send,
                    f_recv.at[sem],
                    (z * CORES + to_core, there),
                ).start()

            if q > 0:
                for e in range(CORES):
                    send(e, 1)
                continue

            @pl.when(k == 0)
            def _():
                send(other, 0)
                finals[0, to_rows, :] = outs[turn, core, from_rows, :]

            @pl.when(k != 0)
            def _():
                send(other, 1)
                send(core, 1)

    act = {"acts": take_acts, "up": multiply, "ring": ring_step, "down": down}
    for name, *at in order():
        act[name](*at)

    def all_of(ref, send, recv):
        return remote(ref, ref, send, recv, partner)

    rest = finals.at[pl.ds(1, NX * NY - 1)]
    near = finals.at[0, pl.ds(pl.multiple_of(other * HALF, HALF), HALF)]
    all_of(near, f_send, f_recv.at[0]).wait_recv()
    all_of(rest, f_send, f_recv.at[1]).wait_recv()

    def total(i, carry):
        rows = pl.ds(pl.multiple_of(i * 16, 16), 16)
        value = finals[0, rows, :].astype(F32)
        for k in range(1, NX * NY):
            value = value + finals[k, rows, :].astype(F32)
        out_ref[rows, :] = value[:, 0:D_ROW].astype(out_ref.dtype)
        return carry

    lax.fori_loop(0, TOK // 16, total, 0)

    swap.wait_send()
    for copy in pushed:
        copy.wait_send()
    all_of(acts.at[pl.ds(HALF, 15 * HALF)], a_send, r_send).wait_send()
    all_of(ring, r_send, h_send).wait_send()
    all_of(hidden.at[pl.ds(0, NZ - 1)], h_send, r_send).wait_send()
    all_of(rest, f_send, r_send).wait_send()
    all_of(near, f_send, r_send).wait_send()


def solution(mesh):
    def step(act_codes, act_scales, gate_weight, up_weight, down_weight):
        dma = pltpu.SemaphoreType.DMA
        return pl.pallas_call(
            kernel,
            out_shape=jax.ShapeDtypeStruct((TOK, D_ROW), BF16),
            in_specs=[pl.BlockSpec(memory_space=pl.ANY)] * 5,
            out_specs=pl.BlockSpec(memory_space=pltpu.VMEM),
            scratch_shapes=[
                pltpu.VMEM((TOK, D_ROW), jnp.int32),
                pltpu.VMEM((TOK, 7), F32),
                pltpu.VMEM((TOK, PAD), BF16),
                pltpu.VMEM((HALF, PAD), BF16),
                pltpu.VMEM((NX * NY * HALF, D_CHIP), BF16),
                pltpu.VMEM((D_CHIP, GU), BF16),
                pltpu.VMEM((CORES, FF, D_ROW), BF16),
                pltpu.VMEM((NQ, ROWS, GU), BF16),
                pltpu.VMEM((2, NQ, LAST, STRIP, GU), BF16),
                pltpu.VMEM((NZ, NQ * PIECE, FF), BF16),
                pltpu.VMEM((NZ, CORES, NQ * PIECE, PAD), BF16),
                pltpu.VMEM((NX * NY, TOK, PAD), BF16),
                dma((2,)),
                dma((5,)),
                dma((5,)),
                dma((5,)),
                dma((2,)),
                dma,
                dma((2, NX * NY)),
                dma,
                dma((2, NQ, LAST)),
                dma,
                dma((2, NQ, HOPS)),
                dma,
                dma((2,)),
            ],
            compiler_params=pltpu.CompilerParams(
                collective_id=0, has_side_effects=True, vmem_limit_bytes=60 * 1024 * 1024
            ),
        )(act_codes, act_scales, gate_weight, up_weight, down_weight)

    return jax.shard_map(
        step,
        mesh=mesh,
        in_specs=(P("col", "row"), P("col", "row"), P("row", "col"), P("row", "col"), P("col", "row")),
        out_specs=P("col", "row"),
        check_vma=False,
    )
```

```python
import functools

import jax
import jax.numpy as jnp
from jax import lax
from jax.experimental import pallas as pl
from jax.experimental.pallas import tpu as pltpu
from jax.sharding import PartitionSpec as P

MESH = pl.DeviceIdType.MESH
F32 = jnp.float32
BF16 = jnp.bfloat16

NZ, NX, NY, CORES = 8, 4, 4, 2
TOK = 128
HALF = TOK // CORES
D_ROW = 448
LOW = 384
D_CHIP = CORES * D_ROW
FF = 1152
GU = 2 * FF
PAD = 512
PIECE = 32
STRIP = 16
QB = 64

GROUPS = (
    ((0, 0), (1, 0), (3, 0), (0, 1)),
    ((0, 3), (1, 1), (3, 3), (1, 3)),
    ((3, 1), (2, 0), (0, 2), (2, 1)),
    ((1, 2), (3, 2), (2, 3), (2, 2)),
)
TURNS = (0, 1, 0, 2, 3, 2, 0, 1, 3, 2, 1, 3, 2, 1, 3, 2, 0, 3, 1, 2, 0, 3, 1, 2, 0, 3, 1, 2, 0, 3, 1, 2, 0, 3, 1, 0)
NQ = len(GROUPS)
SLOT = {s: i for i, s in enumerate(s for g in GROUPS for s in g)}
ROWS = HALF * 4
PASS_ON = {
    (0, 0): ((1, 0), (-1, 0), (0, 1), (0, -1)),
    (1, 0): ((0, 1), (0, -1), (1, 0)),
    (3, 0): ((0, 1), (0, -1)),
    (0, 1): ((0, 1),),
    (1, 1): ((0, 1),),
    (3, 3): ((0, -1),),
    (2, 0): ((0, 1), (0, -1)),
    (2, 3): ((0, -1),),
}
HOPS = NZ // 2
LAST = HOPS


def steps_of(part, slot):
    if part == 0:
        return PASS_ON.get(slot, ())
    return tuple((b, a) for a, b in PASS_ON.get((slot[1], slot[0]), ()))


def length(d, strip):
    return HOPS if strip == d else HOPS - 1


def place(d, strip, hop):
    return hop if strip == d else HOPS + hop


def order():
    near = ((1, 0), (3, 0), (0, 1), (0, 3))
    taken = {(0, 0)}
    ops = []

    def take(slots, late):
        for slot in slots:
            if slot not in taken:
                ops.append(("take", slot, late))
                taken.add(slot)

    at = [0] * NQ
    for q in TURNS:
        stage, at[q] = at[q], at[q] + 1
        if stage == 0:
            if q == 0:
                take(near, True)
                ops += [("pass_on", slot, False) for slot in near]
            take(GROUPS[q], False)
            if q == TURNS[0]:
                ops.append(("weights", 0, 4))
            ops.append(("up", q))
            continue
        ops.append(("ring", q, stage))
        if stage >= LAST:
            if not any(op[0] == "down" for op in ops):
                ops.append(("weights", 4, 5))
            ops.append(("down", q, stage - LAST))
    return ops


def kernel(
    codes, scales, gate_hbm, up_hbm, down_hbm, out_ref,
    staged, swapped, acts, w, wd, part, ring, hidden, outs, finals,
    w_local, w_send, w_recv, swap_sem, a_send, a_recv, r_send, r_recv, h_send, h_recv, f_send, f_recv,
):
    row, col = lax.axis_index("row"), lax.axis_index("col")
    z, core = row // CORES, row % CORES
    y, x = col // NX, col % NX
    other = 1 - core

    def along_z(step):
        return ((z + NZ + step) % NZ * CORES + core, col)

    def in_plane(sx, sy):
        return (row, (y + NY + sy) % NY * NX + (x + NX + sx) % NX)

    partner = (z * CORES + other, col)
    neighbours = (along_z(1), along_z(-1), in_plane(1, 0), in_plane(-1, 0), in_plane(0, 1), in_plane(0, -1))

    def remote(src, dst, send, recv, device):
        return pltpu.make_async_remote_copy(
            src_ref=src, dst_ref=dst, send_sem=send, recv_sem=recv, device_id=device, device_id_type=MESH
        )

    low = pl.ds(pl.multiple_of(core * LOW, 128), LOW)
    tail = pl.ds(pl.multiple_of(CORES * LOW + core * (D_ROW - LOW), 64), D_ROW - LOW)
    pieces = [
        (gate_hbm.at[pl.ds(0, LOW)], w.at[low, pl.ds(0, FF)]),
        (gate_hbm.at[pl.ds(LOW, D_ROW - LOW)], w.at[tail, pl.ds(0, FF)]),
        (up_hbm.at[pl.ds(0, LOW)], w.at[low, pl.ds(FF, FF)]),
        (up_hbm.at[pl.ds(LOW, D_ROW - LOW)], w.at[tail, pl.ds(FF, FF)]),
        (down_hbm, wd.at[core]),
    ]
    local = [pltpu.make_async_copy(src, dst, w_local.at[i]) for i, (src, dst) in enumerate(pieces)]
    pushed = [remote(src, dst, w_send.at[i], w_recv.at[i], partner) for i, (src, dst) in enumerate(pieces)]
    for copy in local:
        copy.start()

    barrier = pltpu.get_barrier_semaphore()
    for device in (partner, *neighbours):
        pl.semaphore_signal(barrier, inc=1, device_id=device, device_id_type=MESH)

    blocks = [
        codes[QB * k : QB * (k + 1), :].astype(F32) * scales[k : k + 1, :] for k in range(D_ROW // QB)
    ]
    blocks.append(jnp.zeros_like(blocks[0]))
    for tile in range(PAD // 128):
        pair = jnp.concatenate(blocks[2 * tile : 2 * tile + 2], axis=0)
        staged[:, tile * 128 : (tile + 1) * 128] = pair.T.astype(BF16)

    pl.semaphore_wait(barrier, 1 + len(neighbours))
    swap = remote(
        staged.at[pl.ds(pl.multiple_of(other * HALF, HALF), HALF)], swapped, swap_sem.at[0], swap_sem.at[1], partner
    )
    swap.start()
    for copy in pushed:
        copy.start()
    swap.wait_recv()
    mine = staged[pl.ds(pl.multiple_of(core * HALF, HALF), HALF), :].astype(F32)
    theirs = swapped[...].astype(F32)
    first = jnp.where(core == 0, mine, theirs)
    second = jnp.where(core == 0, theirs, mine)
    acts[0:HALF, 0:LOW] = first[:, 0:LOW].astype(BF16)
    acts[0:HALF, LOW : 2 * LOW] = second[:, 0:LOW].astype(BF16)
    acts[0:HALF, 2 * LOW : D_CHIP] = (first[:, LOW:PAD] + pltpu.roll(second[:, LOW:PAD], QB, 1)).astype(BF16)

    def acts_rows(slot, half):
        return acts.at[pl.ds(SLOT[slot] * HALF + half * PIECE, PIECE)]

    def pass_on(slot, urgent):
        for half in range(2):
            for sx, sy in steps_of(half, slot):
                there = ((slot[0] + sx) % NX, (slot[1] + sy) % NY)
                if urgent is None or (there in GROUPS[1]) == urgent:
                    remote(
                        acts_rows(slot, half),
                        acts_rows(there, half),
                        a_send,
                        a_recv.at[half, SLOT[there]],
                        in_plane(sx, sy),
                    ).start()

    pass_on((0, 0), None)

    def take_acts(slot, late):
        for half in range(2):
            rows = acts_rows(slot, half)
            remote(rows, rows, a_send, a_recv.at[half, SLOT[slot]], partner).wait_recv()
        pass_on(slot, True if late else None)

    def multiply(q):
        for cut in (pl.ds(0, FF), pl.ds(FF, FF)):
            part[q, :, cut] = jnp.dot(
                acts[q * ROWS : (q + 1) * ROWS, :], w[:, cut], preferred_element_type=F32
            ).astype(BF16)
            for d in range(2):
                for strip in range(2):
                    remote(
                        rows_of(q, strip, z_at(d, length(d, strip))).at[:, cut],
                        ring.at[d, q, place(d, strip, 0), :, cut],
                        r_send,
                        r_recv.at[d, q, place(d, strip, 0)],
                        along_z(toward(d)),
                    ).start()

    def toward(d):
        return 1 - 2 * d

    def z_at(d, hops):
        return (z + NZ + toward(d) * hops) % NZ

    def rows_of(q, strip, owner):
        return part.at[q, pl.ds(pl.multiple_of(owner * PIECE + strip * STRIP, STRIP), STRIP)]

    def arrived(ref, sem):
        remote(ref, ref, r_send, sem, partner).wait_recv()

    def received(q, d, strip, hop):
        ref = ring.at[d, q, place(d, strip, hop)]
        arrived(ref, r_recv.at[d, q, place(d, strip, hop)])
        return ref

    def piece(owner, q):
        return hidden.at[owner, pl.ds(q * PIECE, PIECE)]

    def gather_step(q, hop):
        for d in range(2):
            ref = piece(z_at(d, -hop), q)
            half = hidden.at[z_at(d, -hop), pl.ds(q * PIECE + d * STRIP, STRIP)]
            if hop > 0:
                came = ref if hop < HOPS else half
                arrived(came, h_recv.at[d, q, hop - 1])
            if hop < HOPS:
                goes = ref if hop < HOPS - 1 else half
                remote(goes, goes, h_send, h_recv.at[d, q, hop], along_z(toward(d))).start()

    def ring_step(q, stage):
        if stage < LAST:
            for d in range(2):
                for strip in range(2):
                    left = length(d, strip) - stage
                    if left <= 0:
                        continue
                    got = received(q, d, strip, stage - 1)
                    got[...] = (got[...].astype(F32) + rows_of(q, strip, z_at(d, left))[...].astype(F32)).astype(BF16)
                    at = place(d, strip, stage)
                    remote(got, ring.at[d, q, at], r_send, r_recv.at[d, q, at], along_z(toward(d))).start()
            return
        if stage == LAST:
            for strip in range(2):
                a, b = (received(q, d, strip, length(d, strip) - 1) for d in range(2))
                own = rows_of(q, strip, z)
                gate, up = (
                    a[:, cut].astype(F32) + b[:, cut].astype(F32) + own[:, cut].astype(F32)
                    for cut in (pl.ds(0, FF), pl.ds(FF, FF))
                )
                value = gate / (1.0 + jnp.exp(-gate)) * up
                hidden[z, pl.ds(q * PIECE + strip * STRIP, STRIP), :] = value.astype(BF16)
        gather_step(q, stage - LAST)

    def lookup(q, k, axis):
        packed = sum(s[axis] * 4**i for i, s in enumerate(GROUPS[q]))
        return packed // ((1 + 3 * (k % 2)) * (1 + 15 * (k // 2))) % 4

    def down(q, hop):
        if hop == 0:
            turns = [(0, z)]
        elif hop < HOPS:
            turns = [(2 * hop - 1, (z + NZ - hop) % NZ), (2 * hop, (z + hop) % NZ)]
        else:
            turns = [(NZ - 1, (z + HOPS) % NZ)]
        from_rows = pl.ds(q * PIECE, PIECE)
        value = jnp.concatenate([hidden[owner, from_rows, :] for _, owner in turns], axis=0)
        for e in range(CORES):
            product = lax.dot_general(
                value, wd[e], (((1,), (1,)), ((), ())), preferred_element_type=F32
            ).astype(BF16)
            for i, (turn, _) in enumerate(turns):
                outs[turn, e, from_rows, 0:D_ROW] = product[i * PIECE : (i + 1) * PIECE]
        for turn, owner in turns:
            k = owner // 2
            to_rows = pl.ds(pl.multiple_of(core * HALF + owner % 2 * PIECE, PIECE), PIECE)
            there = (y + NY - lookup(q, k, 1)) % NY * NX + (x + NX - lookup(q, k, 0)) % NX

            def send(to_core, sem):
                remote(
                    outs.at[turn, to_core, from_rows],
                    finals.at[q * 4 + k, to_rows],
                    f_send,
                    f_recv.at[sem],
                    (z * CORES + to_core, there),
                ).start()

            if q > 0:
                for e in range(CORES):
                    send(e, 1)
                continue

            @pl.when(k == 0)
            def _():
                send(other, 0)
                finals[0, to_rows, :] = outs[turn, core, from_rows, :]

            @pl.when(k != 0)
            def _():
                send(other, 1)
                send(core, 1)

    def weights(first, end):
        for i in range(first, end):
            local[i].wait()
            pushed[i].wait_recv()

    act = {"weights": weights, "take": take_acts, "pass_on": pass_on, "up": multiply, "ring": ring_step, "down": down}
    for name, *at in order():
        act[name](*at)

    def all_of(ref, send, recv):
        return remote(ref, ref, send, recv, partner)

    rest = finals.at[pl.ds(1, NX * NY - 1)]
    near = finals.at[0, pl.ds(pl.multiple_of(other * HALF, HALF), HALF)]
    all_of(near, f_send, f_recv.at[0]).wait_recv()
    all_of(rest, f_send, f_recv.at[1]).wait_recv()

    for tile in range(PAD // 128):
        cut = pl.ds(tile * 128, 128)
        value = finals[0, :, cut].astype(F32)
        for k in range(1, NX * NY):
            value = value + finals[k, :, cut].astype(F32)
        rows = min(128, D_ROW - tile * 128)
        out_ref[tile * 128 : tile * 128 + rows, :] = value.T[0:rows, :].astype(out_ref.dtype)

    swap.wait_send()
    for copy in pushed:
        copy.wait_send()
    all_of(acts.at[pl.ds(HALF, 15 * HALF)], a_send, r_send).wait_send()
    all_of(ring, r_send, h_send).wait_send()
    all_of(hidden.at[pl.ds(0, NZ - 1)], h_send, r_send).wait_send()
    all_of(rest, f_send, r_send).wait_send()
    all_of(near, f_send, r_send).wait_send()


def solution(mesh):
    def step(act_codes, act_scales, gate_weight, up_weight, down_weight):
        dma = pltpu.SemaphoreType.DMA
        return pl.pallas_call(
            kernel,
            out_shape=jax.ShapeDtypeStruct((D_ROW, TOK), BF16),
            in_specs=[pl.BlockSpec(memory_space=pltpu.VMEM)] * 2 + [pl.BlockSpec(memory_space=pltpu.HBM)] * 3,
            out_specs=pl.BlockSpec(memory_space=pltpu.VMEM),
            scratch_shapes=[
                pltpu.VMEM((TOK, PAD), BF16),
                pltpu.VMEM((HALF, PAD), BF16),
                pltpu.VMEM((NX * NY * HALF, D_CHIP), BF16),
                pltpu.VMEM((D_CHIP, GU), BF16),
                pltpu.VMEM((CORES, D_ROW, FF), BF16),
                pltpu.VMEM((NQ, ROWS, GU), BF16),
                pltpu.VMEM((2, NQ, NZ - 1, STRIP, GU), BF16),
                pltpu.VMEM((NZ, NQ * PIECE, FF), BF16),
                pltpu.VMEM((NZ, CORES, NQ * PIECE, PAD), BF16),
                pltpu.VMEM((NX * NY, TOK, PAD), BF16),
                dma((5,)),
                dma((5,)),
                dma((5,)),
                dma((2,)),
                dma,
                dma((2, NX * NY)),
                dma,
                dma((2, NQ, NZ - 1)),
                dma,
                dma((2, NQ, HOPS)),
                dma,
                dma((2,)),
            ],
            compiler_params=pltpu.CompilerParams(
                collective_id=0, has_side_effects=True, vmem_limit_bytes=56_000_000
            ),
        )(act_codes.T, act_scales.T, gate_weight, up_weight, down_weight.T).T

    return jax.shard_map(
        step,
        mesh=mesh,
        in_specs=(P("col", "row"), P("col", "row"), P("row", "col"), P("row", "col"), P("col", "row")),
        out_specs=P("col", "row"),
        check_vma=False,
    )
```

```python
import functools

import jax
import jax.numpy as jnp
from jax import lax
from jax.experimental import pallas as pl
from jax.experimental.pallas import tpu as pltpu
from jax.sharding import PartitionSpec as P

MESH = pl.DeviceIdType.MESH
F32 = jnp.float32
BF16 = jnp.bfloat16

NZ, NX, NY, CORES = 8, 4, 4, 2
TOK = 128
HALF = TOK // CORES
D_ROW = 448
LOW = 384
D_CHIP = CORES * D_ROW
FF = 1152
GU = 2 * FF
PAD = 512
PIECE = 32
STRIP = 16
QB = 64

GROUPS = (
    ((0, 0), (1, 0), (3, 0), (0, 1)),
    ((0, 3), (1, 1), (3, 3), (1, 3)),
    ((3, 1), (2, 0), (0, 2), (2, 1)),
    ((1, 2), (3, 2), (2, 3), (2, 2)),
)
TURNS = (0, 1, 0, 2, 3, 2, 0, 1, 3, 2, 1, 3, 2, 1, 3, 2, 0, 3, 1, 2, 0, 3, 1, 2, 0, 3, 1, 2, 0, 3, 1, 2, 0, 3, 1, 0)
NQ = len(GROUPS)
SLOT = {s: i for i, s in enumerate(s for g in GROUPS for s in g)}
ROWS = HALF * 4
PASS_ON = {
    (0, 0): ((1, 0), (-1, 0), (0, 1), (0, -1)),
    (1, 0): ((0, 1), (0, -1), (1, 0)),
    (3, 0): ((0, 1), (0, -1)),
    (0, 1): ((0, 1),),
    (1, 1): ((0, 1),),
    (3, 3): ((0, -1),),
    (2, 0): ((0, 1), (0, -1)),
    (2, 3): ((0, -1),),
}
HOPS = NZ // 2
LAST = HOPS


def steps_of(part, slot):
    if part == 0:
        return PASS_ON.get(slot, ())
    return tuple((b, a) for a, b in PASS_ON.get((slot[1], slot[0]), ()))


def strip_of(kind, d):
    return d if kind == 0 else 1 - d


def place(kind, hop):
    return kind * HOPS + hop


def order():
    near = ((1, 0), (3, 0), (0, 1), (0, 3))
    taken = {(0, 0)}
    ops = []

    def take(slots, late):
        for slot in slots:
            if slot not in taken:
                ops.append(("take", slot, late))
                taken.add(slot)

    at = [0] * NQ
    for q in TURNS:
        stage, at[q] = at[q], at[q] + 1
        if stage == 0:
            if q == 0:
                take(near, True)
                ops += [("pass_on", slot, False) for slot in near]
            take(GROUPS[q], False)
            if q == 2:
                take(GROUPS[3][:3], False)
            if q == TURNS[0]:
                ops.append(("weights", 0))
            ops.append(("up", q))
            continue
        ops.append(("ring", q, stage))
        if stage >= LAST:
            if not any(op[0] == "down" for op in ops):
                ops.append(("weights", 1))
            ops.append(("down", q, stage - LAST))
    return ops


def kernel(
    codes_hbm, scales_hbm, gate_hbm, up_hbm, down_hbm, out_ref,
    codes, scales, staged, swapped, acts, w, wd, part, ring, hidden, outs, finals,
    sent, in_sem, w_local, w_recv, swap_recv, a_recv, r_recv, h_recv, f_recv,
):
    row, col = lax.axis_index("row"), lax.axis_index("col")
    z, core = row // CORES, row % CORES
    y, x = col // NX, col % NX
    other = 1 - core

    def along_z(step):
        return ((z + NZ + step) % NZ * CORES + core, col)

    def in_plane(sx, sy):
        return (row, (y + NY + sy) % NY * NX + (x + NX + sx) % NX)

    partner = (z * CORES + other, col)
    neighbours = (along_z(1), along_z(-1), in_plane(1, 0), in_plane(-1, 0), in_plane(0, 1), in_plane(0, -1))

    def remote(src, dst, recv, device):
        return pltpu.make_async_remote_copy(
            src_ref=src, dst_ref=dst, send_sem=sent, recv_sem=recv, device_id=device, device_id_type=MESH
        )

    def arrived(ref, sem):
        remote(ref, ref, sem, partner).wait_recv()

    in_codes = pltpu.make_async_copy(codes_hbm, codes, in_sem.at[0])
    in_scales = pltpu.make_async_copy(scales_hbm, scales, in_sem.at[1])
    in_codes.start()
    in_scales.start()
    barrier = pltpu.get_barrier_semaphore()
    for device in (partner, *neighbours):
        pl.semaphore_signal(barrier, inc=1, device_id=device, device_id_type=MESH)

    low = pl.ds(pl.multiple_of(core * LOW, 128), LOW)
    tail = pl.ds(pl.multiple_of(CORES * LOW + core * (D_ROW - LOW), 64), D_ROW - LOW)
    pieces = [
        (gate_hbm.at[pl.ds(0, LOW)], w.at[low, pl.ds(0, FF)]),
        (gate_hbm.at[pl.ds(LOW, D_ROW - LOW)], w.at[tail, pl.ds(0, FF)]),
        (up_hbm.at[pl.ds(0, LOW)], w.at[low, pl.ds(FF, FF)]),
        (up_hbm.at[pl.ds(LOW, D_ROW - LOW)], w.at[tail, pl.ds(FF, FF)]),
        (down_hbm, wd.at[core]),
    ]
    for i, (src, dst) in enumerate(pieces):
        pltpu.make_async_copy(src, dst, w_local.at[i // 4]).start()

    in_codes.wait()
    in_scales.wait()
    blocks = [
        codes[QB * k : QB * (k + 1), :].astype(F32) * scales[k : k + 1, :] for k in range(D_ROW // QB)
    ]
    blocks.append(jnp.zeros_like(blocks[0]))
    for tile in range(PAD // 128):
        pair = jnp.concatenate(blocks[2 * tile : 2 * tile + 2], axis=0)
        staged[:, tile * 128 : (tile + 1) * 128] = pair.T.astype(BF16)

    pl.semaphore_wait(barrier, 1 + len(neighbours))
    swap = remote(
        staged.at[pl.ds(pl.multiple_of(other * HALF, HALF), HALF)], swapped, swap_recv, partner
    )
    swap.start()
    for i, (src, dst) in enumerate(pieces):
        remote(src, dst, w_recv.at[i // 4], partner).start()
    swap.wait_recv()
    mine = staged[pl.ds(pl.multiple_of(core * HALF, HALF), HALF), :].astype(F32)
    theirs = swapped[...].astype(F32)
    first = jnp.where(core == 0, mine, theirs)
    second = jnp.where(core == 0, theirs, mine)
    acts[0:HALF, 0:LOW] = first[:, 0:LOW].astype(BF16)
    acts[0:HALF, LOW : 2 * LOW] = second[:, 0:LOW].astype(BF16)
    acts[0:HALF, 2 * LOW : D_CHIP] = (first[:, LOW:PAD] + pltpu.roll(second[:, LOW:PAD], QB, 1)).astype(BF16)

    def acts_rows(slot, half):
        return acts.at[pl.ds(SLOT[slot] * HALF + half * PIECE, PIECE)]

    def pass_on(slot, urgent):
        for half in range(2):
            for sx, sy in steps_of(half, slot):
                there = ((slot[0] + sx) % NX, (slot[1] + sy) % NY)
                if urgent is None or (there in GROUPS[1]) == urgent:
                    remote(
                        acts_rows(slot, half),
                        acts_rows(there, half),
                        a_recv.at[SLOT[there]],
                        in_plane(sx, sy),
                    ).start()

    pass_on((0, 0), None)

    def take_acts(slot, late):
        arrived(acts.at[pl.ds(SLOT[slot] * HALF, HALF)], a_recv.at[SLOT[slot]])
        pass_on(slot, True if late else None)

    def multiply(q):
        for cut in (pl.ds(0, FF), pl.ds(FF, FF)):
            part[q, :, cut] = jnp.dot(
                acts[q * ROWS : (q + 1) * ROWS, :], w[:, cut], preferred_element_type=F32
            ).astype(BF16)
            for kind in range(2):
                for d in range(2):
                    at = place(kind, 0)
                    remote(
                        rows_of(q, strip_of(kind, d), z_at(d, HOPS - kind)).at[:, cut],
                        ring.at[q, at, d, :, cut],
                        r_recv.at[q, at],
                        along_z(toward(d)),
                    ).start()

    def toward(d):
        return 1 - 2 * d

    def z_at(d, hops):
        return (z + NZ + toward(d) * hops) % NZ

    def rows_of(q, strip, owner):
        return part.at[q, pl.ds(pl.multiple_of(owner * PIECE + strip * STRIP, STRIP), STRIP)]

    def received(q, at):
        arrived(ring.at[q, at], r_recv.at[q, at])

    def piece(owner, q):
        return hidden.at[owner, pl.ds(q * PIECE, PIECE)]

    def gather_step(q, hop):
        if hop > 0:
            both = 2 * (PIECE if hop < HOPS else STRIP)
            arrived(hidden.at[0, pl.ds(0, both)], h_recv.at[q, hop - 1])
        if hop < HOPS:
            for d in range(2):
                goes = piece(z_at(d, -hop), q)
                if hop == HOPS - 1:
                    goes = hidden.at[z_at(d, -hop), pl.ds(q * PIECE + d * STRIP, STRIP)]
                remote(goes, goes, h_recv.at[q, hop], along_z(toward(d))).start()

    def ring_step(q, stage):
        if stage < LAST:
            for kind in range(2):
                left = HOPS - kind - stage
                if left <= 0:
                    continue
                at = place(kind, stage)
                received(q, at - 1)
                for d in range(2):
                    got = ring.at[q, at - 1, d]
                    own = rows_of(q, strip_of(kind, d), z_at(d, left))
                    got[...] = (got[...].astype(F32) + own[...].astype(F32)).astype(BF16)
                    remote(got, ring.at[q, at, d], r_recv.at[q, at], along_z(toward(d))).start()
            return
        if stage == LAST:
            ends = [place(kind, HOPS - kind - 1) for kind in range(2)]
            for at in ends:
                received(q, at)
            for strip in range(2):
                a, b = ring.at[q, ends[0], strip], ring.at[q, ends[1], 1 - strip]
                own = rows_of(q, strip, z)
                gate, up = (
                    a[:, cut].astype(F32) + b[:, cut].astype(F32) + own[:, cut].astype(F32)
                    for cut in (pl.ds(0, FF), pl.ds(FF, FF))
                )
                value = gate / (1.0 + jnp.exp(-gate)) * up
                hidden[z, pl.ds(q * PIECE + strip * STRIP, STRIP), :] = value.astype(BF16)
        gather_step(q, stage - LAST)

    def lookup(q, k, axis):
        packed = sum(s[axis] * 4**i for i, s in enumerate(GROUPS[q]))
        return packed // ((1 + 3 * (k % 2)) * (1 + 15 * (k // 2))) % 4

    def down(q, hop):
        if hop == 0:
            turns = [(0, z)]
        elif hop < HOPS:
            turns = [(2 * hop - 1, (z + NZ - hop) % NZ), (2 * hop, (z + hop) % NZ)]
        else:
            turns = [(NZ - 1, (z + HOPS) % NZ)]
        from_rows = pl.ds(q * PIECE, PIECE)
        value = jnp.concatenate([hidden[owner, from_rows, :] for _, owner in turns], axis=0)

        def multiply_by(e):
            product = lax.dot_general(
                value, wd[e], (((1,), (1,)), ((), ())), preferred_element_type=F32
            ).astype(BF16)
            for i, (turn, _) in enumerate(turns):
                outs[turn, e, from_rows, 0:D_ROW] = product[i * PIECE : (i + 1) * PIECE]

        def goes_to(turn, owner):
            k = owner // 2
            to_rows = pl.ds(pl.multiple_of(core * HALF + owner % 2 * PIECE, PIECE), PIECE)
            there = (y + NY - lookup(q, k, 1)) % NY * NX + (x + NX - lookup(q, k, 0)) % NX

            def send(to_core, sem):
                remote(
                    outs.at[turn, to_core, from_rows],
                    finals.at[q * 4 + k, to_rows],
                    f_recv.at[sem],
                    (z * CORES + to_core, there),
                ).start()

            return k, to_rows, send

        for e in range(CORES):
            multiply_by(e)
        for turn, owner in turns:
            k, to_rows, send = goes_to(turn, owner)
            if q > 0:
                for e in range(CORES):
                    send(e, 1)
                continue

            @pl.when(k == 0)
            def _():
                send(other, 0)
                finals[0, to_rows, :] = outs[turn, core, from_rows, :]

            @pl.when(k != 0)
            def _():
                send(other, 1)
                send(core, 1)

    def weights(which):
        ref = w.at[pl.ds(0, D_ROW)] if which == 0 else wd.at[0]
        pltpu.make_async_copy(ref, ref, w_local.at[which]).wait()
        arrived(ref, w_recv.at[which])

    act = {"weights": weights, "take": take_acts, "pass_on": pass_on, "up": multiply, "ring": ring_step, "down": down}
    for name, *at in order():
        act[name](*at)

    rest = finals.at[pl.ds(1, NX * NY - 1)]
    near = finals.at[0, pl.ds(pl.multiple_of(other * HALF, HALF), HALF)]
    arrived(near, f_recv.at[0])
    arrived(rest, f_recv.at[1])

    for tile in range(PAD // 128):
        cut = pl.ds(tile * 128, 128)
        value = finals[0, :, cut].astype(F32)
        for k in range(1, NX * NY):
            value = value + finals[k, :, cut].astype(F32)
        rows = min(128, D_ROW - tile * 128)
        out_ref[tile * 128 : tile * 128 + rows, :] = value.T[0:rows, :].astype(out_ref.dtype)

    for ref in (
        swapped, w.at[pl.ds(0, D_ROW)], wd.at[0], acts.at[pl.ds(HALF, (NX * NY - 1) * HALF)], ring,
        hidden.at[pl.ds(0, NZ - 1)], rest, near,
    ):
        remote(ref, ref, swap_recv, partner).wait_send()


def solution(mesh):
    def step(act_codes, act_scales, gate_weight, up_weight, down_weight):
        dma = pltpu.SemaphoreType.DMA
        return pl.pallas_call(
            kernel,
            out_shape=pltpu.VMEM((D_ROW, TOK), BF16),
            in_specs=[pl.BlockSpec(memory_space=pltpu.HBM)] * 5,
            out_specs=pl.BlockSpec(memory_space=pltpu.VMEM),
            scratch_shapes=[
                pltpu.VMEM((D_ROW, TOK), jnp.int32),
                pltpu.VMEM((7, TOK), F32),
                pltpu.VMEM((TOK, PAD), BF16),
                pltpu.VMEM((HALF, PAD), BF16),
                pltpu.VMEM((NX * NY * HALF, D_CHIP), BF16),
                pltpu.VMEM((D_CHIP, GU), BF16),
                pltpu.VMEM((CORES, D_ROW, FF), BF16),
                pltpu.VMEM((NQ, ROWS, GU), BF16),
                pltpu.VMEM((NQ, NZ - 1, 2, STRIP, GU), BF16),
                pltpu.VMEM((NZ, NQ * PIECE, FF), BF16),
                pltpu.VMEM((NZ, CORES, NQ * PIECE, PAD), BF16),
                pltpu.VMEM((NX * NY, TOK, PAD), BF16),
                dma,
                dma((2,)),
                dma((2,)),
                dma((2,)),
                dma,
                dma((NX * NY,)),
                dma((NQ, NZ - 1)),
                dma((NQ, HOPS)),
                dma((2,)),
            ],
            compiler_params=pltpu.CompilerParams(
                collective_id=0, has_side_effects=True, vmem_limit_bytes=56_000_000
            ),
        )(*(
            pltpu.with_memory_space_constraint(array, pltpu.HBM)
            for array in (act_codes.T, act_scales.T, gate_weight, up_weight, down_weight.T)
        )).T

    return jax.shard_map(
        step,
        mesh=mesh,
        in_specs=(P("col", "row"), P("col", "row"), P("row", "col"), P("row", "col"), P("col", "row")),
        out_specs=P("col", "row"),
        check_vma=False,
    )
```

```python
import functools

import jax
import jax.numpy as jnp
from jax import lax
from jax.experimental import pallas as pl
from jax.experimental.pallas import tpu as pltpu
from jax.sharding import PartitionSpec as P

MESH = pl.DeviceIdType.MESH
F32 = jnp.float32
BF16 = jnp.bfloat16

NZ, NX, NY, CORES = 8, 4, 4, 2
TOK = 128
HALF = TOK // CORES
D_ROW = 448
LOW = 384
D_CHIP = CORES * D_ROW
FF = 1152
GU = 2 * FF
PAD = 512
PIECE = 32
STRIP = 16
QB = 64

GROUPS = (
    ((0, 0), (1, 0), (3, 0), (0, 1)),
    ((0, 3), (1, 1), (3, 3), (1, 3)),
    ((3, 1), (2, 0), (0, 2), (2, 1)),
    ((1, 2), (3, 2), (2, 3), (2, 2)),
)
TURNS = (
    0, 1, 0, 1, 12, 2, 0, 13, 1, 14, 4, 15, 6, 2, 3, 6, 7, 5, 4, 6, 7, 5, 3, 6,
    7, 4, 2, 11, 5, 3, 4, 2, 0, 1, 11, 10, 9, 8, 11, 10, 9, 8, 11, 10, 9, 8, 11, 10,
    9, 8, 10, 9, 8,
)
NQ = len(GROUPS)
SLOT = {s: i for i, s in enumerate(s for g in GROUPS for s in g)}
ROWS = HALF * 4
HROWS = ROWS // 2
PASS_ON = {
    (0, 0): ((1, 0), (-1, 0), (0, 1), (0, -1)),
    (1, 0): ((0, 1), (0, -1), (1, 0)),
    (3, 0): ((0, 1), (0, -1)),
    (0, 1): ((0, 1),),
    (1, 1): ((0, 1),),
    (3, 3): ((0, -1),),
    (2, 0): ((0, 1), (0, -1)),
    (2, 3): ((0, -1),),
}
HOPS = NZ // 2
LAST = HOPS


def steps_of(part, slot):
    if part == 0:
        return PASS_ON.get(slot, ())
    return tuple((b, a) for a, b in PASS_ON.get((slot[1], slot[0]), ()))


NEAR = ((1, 0), (3, 0), (0, 1), (0, 3))
TAKEN = (((1, 1), (3, 3), (1, 3)), ((3, 1), (2, 0), (0, 2)), ((2, 1), (1, 2), (3, 2), (2, 3)), ((2, 2),))


def length(d, strip):
    return HOPS if strip == d else HOPS - 1


def order():
    ops = []
    at = [0 if turn < 2 else turn % 2 for turn in range(2 * NQ)] + [LAST] * NQ
    for turn in TURNS:
        if turn >= 3 * NQ:
            ops += [("take", slot, (0, 1), None) for slot in TAKEN[turn - 3 * NQ]]
            continue
        stage, at[turn] = at[turn], at[turn] + 1
        if stage == 0 and turn < 2:
            ops += [("take", slot, (turn,), True) for slot in NEAR]
            if turn == 0:
                ops.append(("weights", 0))
            else:
                ops += [("pass_on", slot, half, False) for half in range(2) for slot in NEAR]
            ops.append(("up", 0, (turn,)))
        elif stage == 0:
            ops.append(("up", turn // 2, (0, 1)))
        elif turn < 2 * NQ:
            ops.append(("ring", turn // 2, turn % 2, stage))
        else:
            q = turn - 2 * NQ
            if stage == LAST:
                ops.append(("finish", q))
            ops.append(("gather", q, stage - LAST))
            if not any(op[0] == "down" for op in ops):
                ops.append(("weights", 1))
            ops.append(("down", q, stage - LAST))
    return ops


def kernel(
    codes_hbm, scales_hbm, gate_hbm, up_hbm, down_hbm, out_ref,
    codes, scales, staged, swapped, acts, w, wd, part, ring, hidden, outs, finals,
    sent, in_sem, w_local, w_recv, swap_recv, a_recv, r_recv, h_recv, f_recv,
):
    row, col = lax.axis_index("row"), lax.axis_index("col")
    z, core = row // CORES, row % CORES
    y, x = col // NX, col % NX
    other = 1 - core

    def along_z(step):
        return ((z + NZ + step) % NZ * CORES + core, col)

    def in_plane(sx, sy):
        return (row, (y + NY + sy) % NY * NX + (x + NX + sx) % NX)

    partner = (z * CORES + other, col)
    neighbours = (along_z(1), along_z(-1), in_plane(1, 0), in_plane(-1, 0), in_plane(0, 1), in_plane(0, -1))

    def remote(src, dst, recv, device):
        return pltpu.make_async_remote_copy(
            src_ref=src, dst_ref=dst, send_sem=sent, recv_sem=recv, device_id=device, device_id_type=MESH
        )

    def arrived(ref, sem):
        remote(ref, ref, sem, partner).wait_recv()

    in_codes = pltpu.make_async_copy(codes_hbm, codes, in_sem.at[0])
    in_scales = pltpu.make_async_copy(scales_hbm, scales, in_sem.at[1])
    in_codes.start()
    in_scales.start()
    barrier = pltpu.get_barrier_semaphore()
    for device in (partner, *neighbours):
        pl.semaphore_signal(barrier, inc=1, device_id=device, device_id_type=MESH)

    low = pl.ds(pl.multiple_of(core * LOW, 128), LOW)
    tail = pl.ds(pl.multiple_of(CORES * LOW + core * (D_ROW - LOW), 64), D_ROW - LOW)
    pieces = [
        (gate_hbm.at[pl.ds(0, LOW)], w.at[low, pl.ds(0, FF)]),
        (gate_hbm.at[pl.ds(LOW, D_ROW - LOW)], w.at[tail, pl.ds(0, FF)]),
        (up_hbm.at[pl.ds(0, LOW)], w.at[low, pl.ds(FF, FF)]),
        (up_hbm.at[pl.ds(LOW, D_ROW - LOW)], w.at[tail, pl.ds(FF, FF)]),
        (down_hbm, wd.at[core]),
    ]
    for i, (src, dst) in enumerate(pieces):
        pltpu.make_async_copy(src, dst, w_local.at[i // 4]).start()

    in_codes.wait()
    in_scales.wait()
    blocks = [
        codes[QB * k : QB * (k + 1), :].astype(F32) * scales[k : k + 1, :] for k in range(D_ROW // QB)
    ]
    blocks.append(jnp.zeros_like(blocks[0]))
    for tile in range(PAD // 128):
        pair = jnp.concatenate(blocks[2 * tile : 2 * tile + 2], axis=0)
        staged[:, tile * 128 : (tile + 1) * 128] = pair.T.astype(BF16)

    pl.semaphore_wait(barrier, 1 + len(neighbours))
    swap = remote(
        staged.at[pl.ds(pl.multiple_of(other * HALF, HALF), HALF)], swapped, swap_recv, partner
    )
    swap.start()
    for i, (src, dst) in enumerate(pieces):
        remote(src, dst, w_recv.at[i // 4], partner).start()
    swap.wait_recv()
    mine = staged[pl.ds(pl.multiple_of(core * HALF, HALF), HALF), :].astype(F32)
    theirs = swapped[...].astype(F32)
    first = jnp.where(core == 0, mine, theirs)
    second = jnp.where(core == 0, theirs, mine)
    tails = (first[:, LOW:PAD] + pltpu.roll(second[:, LOW:PAD], QB, 1)).astype(BF16)
    for half in range(2):
        there, here = slice(half * HROWS, half * HROWS + PIECE), slice(half * PIECE, (half + 1) * PIECE)
        acts[there, 0:LOW] = first[here, 0:LOW].astype(BF16)
        acts[there, LOW : 2 * LOW] = second[here, 0:LOW].astype(BF16)
        acts[there, 2 * LOW : D_CHIP] = tails[here]

    def acts_rows(slot, half):
        q, k = SLOT[slot] // 4, SLOT[slot] % 4
        return acts.at[pl.ds(q * ROWS + half * HROWS + k * PIECE, PIECE)]

    def acts_sem(slot, half):
        return a_recv.at[NX * NY + NEAR.index(slot) if slot in NEAR and half else SLOT[slot]]

    def pass_on(slot, half, urgent):
        for sx, sy in steps_of(half, slot):
            there = ((slot[0] + sx) % NX, (slot[1] + sy) % NY)
            if urgent is None or (there in GROUPS[1]) == urgent:
                remote(
                    acts_rows(slot, half), acts_rows(there, half), acts_sem(there, half), in_plane(sx, sy)
                ).start()

    for half in range(2):
        pass_on((0, 0), half, None)

    def take_acts(slot, halves, urgent):
        arrived(acts.at[pl.ds(0, len(halves) * PIECE)], acts_sem(slot, halves[0]))
        for half in halves:
            pass_on(slot, half, urgent)

    def multiply(q, strips):
        base, rows = strips[0] * HROWS, len(strips) * HROWS
        for cut in (pl.ds(0, FF), pl.ds(FF, FF)):
            part[q, base : base + rows, cut] = jnp.dot(
                acts[q * ROWS + base : q * ROWS + base + rows, :], w[:, cut], preferred_element_type=F32
            ).astype(BF16)
            for strip in strips:
                for d in range(2):
                    remote(
                        rows_of(q, strip, z_at(d, length(d, strip))).at[:, cut],
                        ring.at[q, strip, 0, d, :, cut],
                        r_recv.at[q, strip, 0],
                        along_z(toward(d)),
                    ).start()

    def toward(d):
        return 1 - 2 * d

    def z_at(d, hops):
        return (z + NZ + toward(d) * hops) % NZ

    def rows_of(q, strip, owner):
        return part.at[q, pl.ds(pl.multiple_of(strip * HROWS + owner * STRIP, STRIP), STRIP)]

    def received(q, strip, hop):
        ref = ring.at[q, strip, hop] if hop < HOPS - 1 else ring.at[q, strip, hop, strip]
        arrived(ref, r_recv.at[q, strip, hop])

    def piece(owner, q):
        return hidden.at[owner, pl.ds(q * PIECE, PIECE)]

    def gather_step(q, hop):
        if hop > 0:
            both = 2 * (PIECE if hop < HOPS else STRIP)
            arrived(hidden.at[0, pl.ds(0, both)], h_recv.at[q, hop - 1])
        if hop < HOPS:
            for d in range(2):
                goes = piece(z_at(d, -hop), q)
                if hop == HOPS - 1:
                    goes = hidden.at[z_at(d, -hop), pl.ds(q * PIECE + d * STRIP, STRIP)]
                remote(goes, goes, h_recv.at[q, hop], along_z(toward(d))).start()

    def ring_step(q, strip, stage):
        received(q, strip, stage - 1)
        for d in range(2):
            left = length(d, strip) - stage
            if left > 0:
                got = ring.at[q, strip, stage - 1, d]
                own = rows_of(q, strip, z_at(d, left))
                got[...] = (got[...].astype(F32) + own[...].astype(F32)).astype(BF16)
                remote(got, ring.at[q, strip, stage, d], r_recv.at[q, strip, stage], along_z(toward(d))).start()

    def finish(q):
        for strip in range(2):
            received(q, strip, HOPS - 1)
            a, b = ring.at[q, strip, HOPS - 1, strip], ring.at[q, strip, HOPS - 2, 1 - strip]
            own = rows_of(q, strip, z)
            gate, up = (
                a[:, cut].astype(F32) + b[:, cut].astype(F32) + own[:, cut].astype(F32)
                for cut in (pl.ds(0, FF), pl.ds(FF, FF))
            )
            value = gate / (1.0 + jnp.exp(-gate)) * up
            hidden[z, pl.ds(q * PIECE + strip * STRIP, STRIP), :] = value.astype(BF16)

    def lookup(q, k, axis):
        packed = sum(s[axis] * 4**i for i, s in enumerate(GROUPS[q]))
        return packed // ((1 + 3 * (k % 2)) * (1 + 15 * (k // 2))) % 4

    def down(q, hop):
        if hop == 0:
            turns = [(0, z)]
        elif hop < HOPS:
            turns = [(2 * hop - 1, (z + NZ - hop) % NZ), (2 * hop, (z + hop) % NZ)]
        else:
            turns = [(NZ - 1, (z + HOPS) % NZ)]
        from_rows = pl.ds(q * PIECE, PIECE)
        value = jnp.concatenate([hidden[owner, from_rows, :] for _, owner in turns], axis=0)

        def multiply_by(e):
            product = lax.dot_general(
                value, wd[e], (((1,), (1,)), ((), ())), preferred_element_type=F32
            ).astype(BF16)
            for i, (turn, _) in enumerate(turns):
                outs[turn, e, from_rows, 0:D_ROW] = product[i * PIECE : (i + 1) * PIECE]

        def goes_to(turn, owner):
            k = owner // 2
            to_rows = pl.ds(pl.multiple_of(core * HALF + owner % 2 * PIECE, PIECE), PIECE)
            there = (y + NY - lookup(q, k, 1)) % NY * NX + (x + NX - lookup(q, k, 0)) % NX

            def send(to_core, sem):
                remote(
                    outs.at[turn, to_core, from_rows],
                    finals.at[q * 4 + k, to_rows],
                    f_recv.at[sem],
                    (z * CORES + to_core, there),
                ).start()

            return k, to_rows, send

        for e in range(CORES):
            multiply_by(e)
        for turn, owner in turns:
            k, to_rows, send = goes_to(turn, owner)
            if q > 0:
                for e in range(CORES):
                    send(e, 1)
                continue

            @pl.when(k == 0)
            def _():
                send(other, 0)
                finals[0, to_rows, :] = outs[turn, core, from_rows, :]

            @pl.when(k != 0)
            def _():
                send(other, 1)
                send(core, 1)

    def weights(which):
        ref = w.at[pl.ds(0, D_ROW)] if which == 0 else wd.at[0]
        pltpu.make_async_copy(ref, ref, w_local.at[which]).wait()
        arrived(ref, w_recv.at[which])

    act = {
        "weights": weights, "take": take_acts, "pass_on": pass_on, "up": multiply, "ring": ring_step,
        "finish": finish, "gather": gather_step, "down": down,
    }
    for name, *at in order():
        act[name](*at)

    rest = finals.at[pl.ds(1, NX * NY - 1)]
    near = finals.at[0, pl.ds(pl.multiple_of(other * HALF, HALF), HALF)]
    arrived(near, f_recv.at[0])
    arrived(rest, f_recv.at[1])

    for tile in range(PAD // 128):
        cut = pl.ds(tile * 128, 128)
        value = finals[0, :, cut].astype(F32)
        for k in range(1, NX * NY):
            value = value + finals[k, :, cut].astype(F32)
        value = jnp.concatenate([value[STRIP * i : STRIP * (i + 1)] for i in (0, 2, 1, 3, 4, 6, 5, 7)], axis=0)
        rows = min(128, D_ROW - tile * 128)
        out_ref[tile * 128 : tile * 128 + rows, :] = value.T[0:rows, :].astype(out_ref.dtype)

    for ref in (
        swapped, w.at[pl.ds(0, D_ROW)], wd.at[0], acts.at[pl.ds(HALF, (NX * NY - 1) * HALF)],
        ring.at[pl.ds(0, NQ - 1)], ring.at[NQ - 1, 0], hidden.at[pl.ds(0, NZ - 1)], rest, near,
    ):
        remote(ref, ref, swap_recv, partner).wait_send()


def solution(mesh):
    def step(act_codes, act_scales, gate_weight, up_weight, down_weight):
        dma = pltpu.SemaphoreType.DMA
        return pl.pallas_call(
            kernel,
            out_shape=pltpu.VMEM((D_ROW, TOK), BF16),
            in_specs=[pl.BlockSpec(memory_space=pltpu.HBM)] * 5,
            out_specs=pl.BlockSpec(memory_space=pltpu.VMEM),
            scratch_shapes=[
                pltpu.VMEM((D_ROW, TOK), jnp.int32),
                pltpu.VMEM((7, TOK), F32),
                pltpu.VMEM((TOK, PAD), BF16),
                pltpu.VMEM((HALF, PAD), BF16),
                pltpu.VMEM((NX * NY * HALF, D_CHIP), BF16),
                pltpu.VMEM((D_CHIP, GU), BF16),
                pltpu.VMEM((CORES, D_ROW, FF), BF16),
                pltpu.VMEM((NQ, ROWS, GU), BF16),
                pltpu.VMEM((NQ, 2, HOPS, 2, STRIP, GU), BF16),
                pltpu.VMEM((NZ, NQ * PIECE, FF), BF16),
                pltpu.VMEM((NZ, CORES, NQ * PIECE, PAD), BF16),
                pltpu.VMEM((NX * NY, TOK, PAD), BF16),
                dma,
                dma((2,)),
                dma((2,)),
                dma((2,)),
                dma,
                dma((NX * NY + len(NEAR),)),
                dma((NQ, 2, HOPS)),
                dma((NQ, HOPS)),
                dma((2,)),
            ],
            compiler_params=pltpu.CompilerParams(
                collective_id=0, has_side_effects=True, vmem_limit_bytes=56_000_000
            ),
        )(*(
            pltpu.with_memory_space_constraint(array, pltpu.HBM)
            for array in (act_codes.T, act_scales.T, gate_weight, up_weight, down_weight.T)
        )).T

    return jax.shard_map(
        step,
        mesh=mesh,
        in_specs=(P("col", "row"), P("col", "row"), P("row", "col"), P("row", "col"), P("col", "row")),
        out_specs=P("col", "row"),
        check_vma=False,
    )
```

```python
import functools

import jax
import jax.numpy as jnp
from jax import lax
from jax.experimental import pallas as pl
from jax.experimental.pallas import tpu as pltpu
from jax.sharding import PartitionSpec as P

MESH = pl.DeviceIdType.MESH
F32 = jnp.float32
BF16 = jnp.bfloat16

NZ, NX, NY, CORES = 8, 4, 4, 2
TOK = 128
HALF = TOK // CORES
D_ROW = 448
LOW = 384
D_CHIP = CORES * D_ROW
FF = 1152
GU = 2 * FF
PAD = 512
PIECE = 32
STRIP = 16
QB = 64

GROUPS = (
    ((0, 0), (1, 0), (3, 0), (0, 1)),
    ((0, 3), (1, 1), (3, 3), (1, 3)),
    ((3, 1), (2, 0), (0, 2), (2, 1)),
    ((1, 2), (3, 2), (2, 3), (2, 2)),
)
TURNS = (
    0, 1, 0, 1, 12, 2, 0, 13, 1, 14, 4, 15, 6, 2, 3, 6, 7, 5, 4, 6, 7, 5, 3, 6,
    7, 4, 2, 11, 5, 3, 4, 2, 0, 1, 11, 10, 9, 8, 11, 10, 9, 8, 11, 10, 9, 8, 11, 10,
    9, 8, 10, 9, 8,
)
NQ = len(GROUPS)
SLOT = {s: i for i, s in enumerate(s for g in GROUPS for s in g)}
ROWS = HALF * 4
HROWS = ROWS // 2
PASS_ON = {
    (0, 0): ((1, 0), (-1, 0), (0, 1), (0, -1)),
    (1, 0): ((0, 1), (0, -1), (1, 0)),
    (3, 0): ((0, 1), (0, -1)),
    (0, 1): ((0, 1),),
    (1, 1): ((0, 1),),
    (3, 3): ((0, -1),),
    (2, 0): ((0, 1), (0, -1)),
    (2, 3): ((0, -1),),
}
HOPS = NZ // 2
LAST = HOPS


def steps_of(part, slot):
    if part == 0:
        return PASS_ON.get(slot, ())
    return tuple((b, a) for a, b in PASS_ON.get((slot[1], slot[0]), ()))


NEAR = ((1, 0), (3, 0), (0, 1), (0, 3))
TAKEN = (((1, 1), (3, 3), (1, 3)), ((3, 1), (2, 0), (0, 2)), ((2, 1), (1, 2), (3, 2), (2, 3)), ((2, 2),))


def length(d, strip):
    return HOPS if strip == d else HOPS - 1


def order():
    ops = []
    at = [0 if turn < 2 else turn % 2 for turn in range(2 * NQ)] + [LAST] * NQ
    for turn in TURNS:
        if turn >= 3 * NQ:
            ops.append(("take", TAKEN[turn - 3 * NQ], (0, 1), None))
            continue
        stage, at[turn] = at[turn], at[turn] + 1
        if stage == 0 and turn < 2:
            ops += [("take", slots, (turn,), True) for slots in ([(slot,) for slot in NEAR] if turn == 0 else [NEAR])]
            if turn == 0:
                ops.append(("weights", 0))
            else:
                ops += [("pass_on", slot, half, False) for half in range(2) for slot in NEAR]
            ops.append(("up", 0, (turn,)))
        elif stage == 0:
            ops.append(("up", turn // 2, (0, 1)))
        elif turn < 2 * NQ:
            ops.append(("ring", turn // 2, turn % 2, stage))
            if turn // 2 == 3 and stage == 1 and ("weights", 1) not in ops:
                ops.append(("weights", 1))
        else:
            q = turn - 2 * NQ
            if stage == LAST:
                ops.append(("finish", q))
            ops.append(("gather", q, stage - LAST))
            ops.append(("down", q, stage - LAST))
    return ops


def kernel(
    codes_hbm, scales_hbm, gate_hbm, up_hbm, down_hbm, out_ref,
    codes, scales, staged, swapped, acts, w, wd, part, ring, hidden, outs, finals, sums, wdt,
    sent, in_sem, w_local, w_recv, swap_recv, a_recv, r_recv, h_recv, f_recv,
):
    row, col = lax.axis_index("row"), lax.axis_index("col")
    z, core = row // CORES, row % CORES
    y, x = col // NX, col % NX
    other = 1 - core

    def along_z(step):
        return ((z + NZ + step) % NZ * CORES + core, col)

    def in_plane(sx, sy):
        return (row, (y + NY + sy) % NY * NX + (x + NX + sx) % NX)

    partner = (z * CORES + other, col)
    neighbours = (along_z(1), along_z(-1), in_plane(1, 0), in_plane(-1, 0), in_plane(0, 1), in_plane(0, -1))

    def remote(src, dst, recv, device):
        return pltpu.make_async_remote_copy(
            src_ref=src, dst_ref=dst, send_sem=sent, recv_sem=recv, device_id=device, device_id_type=MESH
        )

    def arrived(ref, sem):
        remote(ref, ref, sem, partner).wait_recv()

    in_codes = pltpu.make_async_copy(codes_hbm, codes, in_sem.at[0])
    in_scales = pltpu.make_async_copy(scales_hbm, scales, in_sem.at[1])
    in_codes.start()
    in_scales.start()
    barrier = pltpu.get_barrier_semaphore()
    for device in (partner, *neighbours):
        pl.semaphore_signal(barrier, inc=1, device_id=device, device_id_type=MESH)

    low = pl.ds(pl.multiple_of(core * LOW, 128), LOW)
    tail = pl.ds(pl.multiple_of(CORES * LOW + core * (D_ROW - LOW), 64), D_ROW - LOW)
    pieces = [
        (gate_hbm.at[pl.ds(0, LOW)], w.at[low, pl.ds(0, FF)]),
        (gate_hbm.at[pl.ds(LOW, D_ROW - LOW)], w.at[tail, pl.ds(0, FF)]),
        (up_hbm.at[pl.ds(0, LOW)], w.at[low, pl.ds(FF, FF)]),
        (up_hbm.at[pl.ds(LOW, D_ROW - LOW)], w.at[tail, pl.ds(FF, FF)]),
        (down_hbm, wd.at[core]),
    ]
    for i, (src, dst) in enumerate(pieces):
        pltpu.make_async_copy(src, dst, w_local.at[i // 4]).start()

    in_codes.wait()
    in_scales.wait()
    blocks = [
        codes[QB * k : QB * (k + 1), :].astype(F32) * scales[k : k + 1, :] for k in range(D_ROW // QB)
    ]
    blocks.append(jnp.zeros_like(blocks[0]))
    for tile in range(PAD // 128):
        pair = jnp.concatenate(blocks[2 * tile : 2 * tile + 2], axis=0)
        staged[:, tile * 128 : (tile + 1) * 128] = pair.T.astype(BF16)

    pl.semaphore_wait(barrier, 1 + len(neighbours))
    swap = remote(
        staged.at[pl.ds(pl.multiple_of(other * HALF, HALF), HALF)], swapped, swap_recv, partner
    )
    swap.start()
    for i, (src, dst) in enumerate(pieces):
        remote(src, dst, w_recv.at[i // 4], partner).start()
    swap.wait_recv()
    mine = staged[pl.ds(pl.multiple_of(core * HALF, HALF), HALF), :].astype(F32)
    theirs = swapped[...].astype(F32)
    first = jnp.where(core == 0, mine, theirs)
    second = jnp.where(core == 0, theirs, mine)
    tails = (first[:, LOW:PAD] + pltpu.roll(second[:, LOW:PAD], QB, 1)).astype(BF16)
    for half in range(2):
        there, here = slice(half * HROWS, half * HROWS + PIECE), slice(half * PIECE, (half + 1) * PIECE)
        acts[there, 0:LOW] = first[here, 0:LOW].astype(BF16)
        acts[there, LOW : 2 * LOW] = second[here, 0:LOW].astype(BF16)
        acts[there, 2 * LOW : D_CHIP] = tails[here]

    def acts_rows(slot, half):
        q, k = SLOT[slot] // 4, SLOT[slot] % 4
        return acts.at[pl.ds(q * ROWS + half * HROWS + k * PIECE, PIECE)]

    def acts_sem(slot, half):
        if slot in NEAR:
            return a_recv.at[len(NEAR) if half else NEAR.index(slot)]
        return a_recv.at[len(NEAR) + 1 + next(i for i, slots in enumerate(TAKEN) if slot in slots)]

    def pass_on(slot, half, urgent):
        for sx, sy in steps_of(half, slot):
            there = ((slot[0] + sx) % NX, (slot[1] + sy) % NY)
            if urgent is None or (there in GROUPS[1]) == urgent:
                remote(
                    acts_rows(slot, half), acts_rows(there, half), acts_sem(there, half), in_plane(sx, sy)
                ).start()

    for half in range(2):
        pass_on((0, 0), half, None)

    def take_acts(slots, halves, urgent):
        arrived(acts.at[pl.ds(0, len(slots) * len(halves) * PIECE)], acts_sem(slots[0], halves[0]))
        for slot in slots:
            for half in halves:
                pass_on(slot, half, urgent)

    def multiply(q, strips):
        base, rows = strips[0] * HROWS, len(strips) * HROWS
        for cut in (pl.ds(0, FF), pl.ds(FF, FF)):
            part[q, base : base + rows, cut] = jnp.dot(
                acts[q * ROWS + base : q * ROWS + base + rows, :], w[:, cut], preferred_element_type=F32
            ).astype(BF16)
            for strip in strips:
                for d in range(2):
                    remote(
                        rows_of(q, strip, z_at(d, length(d, strip))).at[:, cut],
                        ring.at[q, strip, 0, d, :, cut],
                        r_recv.at[q, strip, 0],
                        along_z(toward(d)),
                    ).start()

    def toward(d):
        return 1 - 2 * d

    def z_at(d, hops):
        return (z + NZ + toward(d) * hops) % NZ

    def rows_of(q, strip, owner):
        return part.at[q, pl.ds(pl.multiple_of(strip * HROWS + owner * STRIP, STRIP), STRIP)]

    def received(q, strip, hop):
        ref = ring.at[q, strip, hop] if hop < HOPS - 1 else ring.at[q, strip, hop, strip]
        arrived(ref, r_recv.at[q, strip, hop])

    def piece(owner, q):
        return hidden.at[owner, pl.ds(q * PIECE, PIECE)]

    def gather_step(q, hop):
        if hop > 0:
            both = 2 * (PIECE if hop < HOPS else STRIP)
            arrived(hidden.at[0, pl.ds(0, both)], h_recv.at[q, hop - 1])
        if hop < HOPS:
            for d in range(2):
                goes = piece(z_at(d, -hop), q)
                if hop == HOPS - 1:
                    goes = hidden.at[z_at(d, -hop), pl.ds(q * PIECE + d * STRIP, STRIP)]
                remote(goes, goes, h_recv.at[q, hop], along_z(toward(d))).start()

    def ring_step(q, strip, stage):
        received(q, strip, stage - 1)
        for d in range(2):
            left = length(d, strip) - stage
            if left > 0:
                got = ring.at[q, strip, stage - 1, d]
                own = rows_of(q, strip, z_at(d, left))
                got[...] = (got[...].astype(F32) + own[...].astype(F32)).astype(BF16)
                remote(got, ring.at[q, strip, stage, d], r_recv.at[q, strip, stage], along_z(toward(d))).start()

    def finish(q):
        for strip in range(2):
            received(q, strip, HOPS - 1)
            a, b = ring.at[q, strip, HOPS - 1, strip], ring.at[q, strip, HOPS - 2, 1 - strip]
            own = rows_of(q, strip, z)
            gate, up = (
                a[:, cut].astype(F32) + b[:, cut].astype(F32) + own[:, cut].astype(F32)
                for cut in (pl.ds(0, FF), pl.ds(FF, FF))
            )
            value = gate / (1.0 + jnp.exp(-gate)) * up
            hidden[z, pl.ds(q * PIECE + strip * STRIP, STRIP), :] = value.astype(BF16)

    def lookup(q, k, axis):
        packed = sum(s[axis] * 4**i for i, s in enumerate(GROUPS[q]))
        return packed // ((1 + 3 * (k % 2)) * (1 + 15 * (k // 2))) % 4

    def down(q, hop):
        if hop == 0:
            turns = [(0, z)]
        elif hop < HOPS:
            turns = [(2 * hop - 1, (z + NZ - hop) % NZ), (2 * hop, (z + hop) % NZ)]
        else:
            turns = [(NZ - 1, (z + HOPS) % NZ)]
        from_rows = pl.ds(q * PIECE, PIECE)
        value = jnp.concatenate([hidden[owner, from_rows, :] for _, owner in turns], axis=0)

        def multiply_by(e):
            product = jnp.dot(value, wdt[e], preferred_element_type=F32).astype(BF16)
            for i, (turn, _) in enumerate(turns):
                outs[turn, e, from_rows, 0:D_ROW] = product[i * PIECE : (i + 1) * PIECE]

        def goes_to(turn, owner):
            k = owner // 2
            to_rows = pl.ds(pl.multiple_of(core * HALF + owner % 2 * PIECE, PIECE), PIECE)
            there = (y + NY - lookup(q, k, 1)) % NY * NX + (x + NX - lookup(q, k, 0)) % NX

            def send(to_core, sem=1 + q):
                remote(
                    outs.at[turn, to_core, from_rows],
                    finals.at[q * 4 + k, to_rows],
                    f_recv.at[sem],
                    (z * CORES + to_core, there),
                ).start()

            return k, to_rows, send

        for e in range(CORES):
            multiply_by(e)
        for turn, owner in turns:
            k, to_rows, send = goes_to(turn, owner)
            if q > 0:
                for e in range(CORES):
                    send(e)
                continue

            @pl.when(k == 0)
            def _():
                send(other, 0)
                finals[0, to_rows, :] = outs[turn, core, from_rows, :]

            @pl.when(k != 0)
            def _():
                send(other)
                send(core)

    def weights(which):
        ref = w.at[pl.ds(0, D_ROW)] if which == 0 else wd.at[0]
        pltpu.make_async_copy(ref, ref, w_local.at[which]).wait()
        arrived(ref, w_recv.at[which])
        if which == 1:
            for e in range(CORES):
                for tile in range(FF // 128):
                    cut = slice(tile * 128, (tile + 1) * 128)
                    wdt[e, cut, :] = wd[e, :, cut].astype(F32).T.astype(BF16)

    act = {
        "weights": weights, "take": take_acts, "pass_on": pass_on, "up": multiply, "ring": ring_step,
        "finish": finish, "gather": gather_step, "down": down,
    }
    for name, *at in order():
        act[name](*at)

    rest = finals.at[pl.ds(1, NX * NY - 1)]
    near = finals.at[0, pl.ds(pl.multiple_of(other * HALF, HALF), HALF)]
    for q in reversed(range(NQ)):
        first = 4 * q
        if q == 0:
            arrived(near, f_recv.at[0])
            arrived(finals.at[pl.ds(1, 3)], f_recv.at[1])
        else:
            arrived(finals.at[pl.ds(first, 4)], f_recv.at[1 + q])
        for tile in range(PAD // 128):
            cut = pl.ds(tile * 128, 128)
            value = finals[first, :, cut].astype(F32)
            for k in range(first + 1, first + 4):
                value = value + finals[k, :, cut].astype(F32)
            if q < NQ - 1:
                value = value + sums[:, cut]
            if q > 0:
                sums[:, cut] = value
                continue
            value = jnp.concatenate([value[STRIP * i : STRIP * (i + 1)] for i in (0, 2, 1, 3, 4, 6, 5, 7)], axis=0)
            rows = min(128, D_ROW - tile * 128)
            out_ref[tile * 128 : tile * 128 + rows, :] = value.T[0:rows, :].astype(out_ref.dtype)

    for ref in (
        swapped, w.at[pl.ds(0, D_ROW)], wd.at[0], acts.at[pl.ds(HALF, (NX * NY - 1) * HALF)],
        ring.at[pl.ds(0, NQ - 1)], ring.at[NQ - 1, 0], hidden.at[pl.ds(0, NZ - 1)], rest, near,
    ):
        remote(ref, ref, swap_recv, partner).wait_send()


def solution(mesh):
    def step(act_codes, act_scales, gate_weight, up_weight, down_weight):
        dma = pltpu.SemaphoreType.DMA
        return pl.pallas_call(
            kernel,
            out_shape=pltpu.VMEM((D_ROW, TOK), BF16),
            in_specs=[pl.BlockSpec(memory_space=pltpu.HBM)] * 5,
            out_specs=pl.BlockSpec(memory_space=pltpu.VMEM),
            scratch_shapes=[
                pltpu.VMEM((D_ROW, TOK), jnp.int32),
                pltpu.VMEM((7, TOK), F32),
                pltpu.VMEM((TOK, PAD), BF16),
                pltpu.VMEM((HALF, PAD), BF16),
                pltpu.VMEM((NX * NY * HALF, D_CHIP), BF16),
                pltpu.VMEM((D_CHIP, GU), BF16),
                pltpu.VMEM((CORES, D_ROW, FF), BF16),
                pltpu.VMEM((NQ, ROWS, GU), BF16),
                pltpu.VMEM((NQ, 2, HOPS, 2, STRIP, GU), BF16),
                pltpu.VMEM((NZ, NQ * PIECE, FF), BF16),
                pltpu.VMEM((NZ, CORES, NQ * PIECE, PAD), BF16),
                pltpu.VMEM((NX * NY, TOK, PAD), BF16),
                pltpu.VMEM((TOK, PAD), F32),
                pltpu.VMEM((CORES, FF, D_ROW), BF16),
                dma,
                dma((2,)),
                dma((2,)),
                dma((2,)),
                dma,
                dma((len(NEAR) + 1 + len(TAKEN),)),
                dma((NQ, 2, HOPS)),
                dma((NQ, HOPS)),
                dma((1 + NQ,)),
            ],
            compiler_params=pltpu.CompilerParams(
                collective_id=0, has_side_effects=True, vmem_limit_bytes=56_000_000
            ),
        )(*(
            pltpu.with_memory_space_constraint(array, pltpu.HBM)
            for array in (act_codes.T, act_scales.T, gate_weight, up_weight, down_weight.T)
        )).T

    return jax.shard_map(
        step,
        mesh=mesh,
        in_specs=(P("col", "row"), P("col", "row"), P("row", "col"), P("row", "col"), P("col", "row")),
        out_specs=P("col", "row"),
        check_vma=False,
    )
```

```python
import functools

import jax
import jax.numpy as jnp
from jax import lax
from jax.experimental import pallas as pl
from jax.experimental.pallas import tpu as pltpu
from jax.sharding import PartitionSpec as P

MESH = pl.DeviceIdType.MESH
F32 = jnp.float32
BF16 = jnp.bfloat16

NZ, NX, NY, CORES = 8, 4, 4, 2
TOK = 128
HALF = TOK // CORES
D_ROW = 448
LOW = 384
D_CHIP = CORES * D_ROW
FF = 1152
GU = 2 * FF
PAD = 512
PIECE = 32
STRIP = 16
QB = 64

GROUPS = (
    ((0, 0), (1, 0), (3, 0), (0, 1)),
    ((0, 3), (1, 1), (3, 3), (1, 3)),
    ((3, 1), (2, 0), (0, 2), (2, 1)),
    ((1, 2), (3, 2), (2, 3), (2, 2)),
)
TURNS = (
    0, 1, 0, 1, 12, 2, 0, 13, 1, 14, 4, 15, 6, 2, 3, 6, 7, 5, 4, 6, 7, 5, 3, 6,
    7, 4, 2, 11, 5, 3, 4, 2, 0, 1, 11, 10, 9, 8, 11, 10, 9, 8, 11, 10, 9, 8, 11, 10,
    9, 8, 10, 9, 8,
)
NQ = len(GROUPS)
SLOT = {s: i for i, s in enumerate(s for g in GROUPS for s in g)}
ROWS = HALF * 4
HROWS = ROWS // 2
PASS_ON = {
    (0, 0): ((1, 0), (-1, 0), (0, 1), (0, -1)),
    (1, 0): ((0, 1), (0, -1), (1, 0)),
    (3, 0): ((0, 1), (0, -1)),
    (0, 1): ((0, 1),),
    (1, 1): ((0, 1),),
    (3, 3): ((0, -1),),
    (2, 0): ((0, 1), (0, -1)),
    (2, 3): ((0, -1),),
}
HOPS = NZ // 2
LAST = HOPS


def steps_of(part, slot):
    if part == 0:
        return PASS_ON.get(slot, ())
    return tuple((b, a) for a, b in PASS_ON.get((slot[1], slot[0]), ()))


NEAR = ((1, 0), (3, 0), (0, 1), (0, 3))
TAKEN = (((1, 1), (3, 3), (1, 3)), ((3, 1), (2, 0), (0, 2)), ((2, 1), (1, 2), (3, 2), (2, 3)), ((2, 2),))


def length(d, strip):
    return HOPS if strip == d else HOPS - 1


def order():
    ops = []
    at = [0 if turn < 2 else turn % 2 for turn in range(2 * NQ)] + [LAST] * NQ
    for turn in TURNS:
        if turn >= 3 * NQ:
            ops.append(("take", TAKEN[turn - 3 * NQ], (0, 1), None))
            continue
        stage, at[turn] = at[turn], at[turn] + 1
        if stage == 0 and turn < 2:
            ops += [("take", slots, (turn,), True) for slots in ([(slot,) for slot in NEAR[:3]] if turn == 0 else [NEAR])]
            if turn == 0:
                ops.append(("weights", 0))
            else:
                ops += [("pass_on", slot, half, False) for half in range(2) for slot in NEAR]
            ops.append(("up", 0, (turn,)))
            if turn == 1:
                ops.append(("take", NEAR[3:], (0,), True))
        elif stage == 0:
            ops.append(("up", turn // 2, (0, 1)))
        elif turn < 2 * NQ:
            ops.append(("ring", turn // 2, turn % 2, stage))
            if turn // 2 == 3 and stage == 1 and ("weights", 1) not in ops:
                ops.append(("weights", 1))
        else:
            q = turn - 2 * NQ
            if stage == LAST:
                ops.append(("finish", q))
            ops.append(("gather", q, stage - LAST))
            ops.append(("down", q, stage - LAST))
    return ops


def kernel(
    codes_hbm, scales_hbm, gate_hbm, up_hbm, down_hbm, out_ref,
    codes, scales, staged, swapped, acts, w, wd, part, ring, hidden, outs, finals, sums, wdt,
    sent, in_sem, w_local, w_recv, swap_recv, a_recv, r_recv, h_recv, f_recv,
):
    row, col = lax.axis_index("row"), lax.axis_index("col")
    z, core = row // CORES, row % CORES
    y, x = col // NX, col % NX
    other = 1 - core

    def along_z(step):
        return ((z + NZ + step) % NZ * CORES + core, col)

    def in_plane(sx, sy):
        return (row, (y + NY + sy) % NY * NX + (x + NX + sx) % NX)

    partner = (z * CORES + other, col)
    neighbours = (along_z(1), along_z(-1), in_plane(1, 0), in_plane(-1, 0), in_plane(0, 1), in_plane(0, -1))

    def remote(src, dst, recv, device):
        return pltpu.make_async_remote_copy(
            src_ref=src, dst_ref=dst, send_sem=sent, recv_sem=recv, device_id=device, device_id_type=MESH
        )

    def arrived(ref, sem):
        remote(ref, ref, sem, partner).wait_recv()

    in_codes = pltpu.make_async_copy(codes_hbm, codes, in_sem.at[0])
    in_scales = pltpu.make_async_copy(scales_hbm, scales, in_sem.at[1])
    in_codes.start()
    in_scales.start()
    barrier = pltpu.get_barrier_semaphore()
    for device in (partner, *neighbours):
        pl.semaphore_signal(barrier, inc=1, device_id=device, device_id_type=MESH)

    low = pl.ds(pl.multiple_of(core * LOW, 128), LOW)
    tail = pl.ds(pl.multiple_of(CORES * LOW + core * (D_ROW - LOW), 64), D_ROW - LOW)
    pieces = [
        (gate_hbm.at[pl.ds(0, LOW)], w.at[low, pl.ds(0, FF)]),
        (gate_hbm.at[pl.ds(LOW, D_ROW - LOW)], w.at[tail, pl.ds(0, FF)]),
        (up_hbm.at[pl.ds(0, LOW)], w.at[low, pl.ds(FF, FF)]),
        (up_hbm.at[pl.ds(LOW, D_ROW - LOW)], w.at[tail, pl.ds(FF, FF)]),
        (down_hbm, wd.at[core]),
    ]
    for i, (src, dst) in enumerate(pieces):
        pltpu.make_async_copy(src, dst, w_local.at[i // 4]).start()

    in_codes.wait()
    in_scales.wait()
    blocks = [
        codes[QB * k : QB * (k + 1), :].astype(F32) * scales[k : k + 1, :] for k in range(D_ROW // QB)
    ]
    blocks.append(jnp.zeros_like(blocks[0]))
    for tile in range(PAD // 128):
        pair = jnp.concatenate(blocks[2 * tile : 2 * tile + 2], axis=0)
        staged[:, tile * 128 : (tile + 1) * 128] = pair.T.astype(BF16)

    pl.semaphore_wait(barrier, 1 + len(neighbours))
    swap = remote(
        staged.at[pl.ds(pl.multiple_of(other * HALF, HALF), HALF)], swapped, swap_recv, partner
    )
    swap.start()
    for i, (src, dst) in enumerate(pieces):
        remote(src, dst, w_recv.at[i // 4], partner).start()
    swap.wait_recv()
    mine = staged[pl.ds(pl.multiple_of(core * HALF, HALF), HALF), :].astype(F32)
    theirs = swapped[...].astype(F32)
    first = jnp.where(core == 0, mine, theirs)
    second = jnp.where(core == 0, theirs, mine)
    tails = (first[:, LOW:PAD] + pltpu.roll(second[:, LOW:PAD], QB, 1)).astype(BF16)
    for half in range(2):
        there, here = slice(half * HROWS, half * HROWS + PIECE), slice(half * PIECE, (half + 1) * PIECE)
        acts[there, 0:LOW] = first[here, 0:LOW].astype(BF16)
        acts[there, LOW : 2 * LOW] = second[here, 0:LOW].astype(BF16)
        acts[there, 2 * LOW : D_CHIP] = tails[here]

    def acts_rows(slot, half):
        q, k = SLOT[slot] // 4, SLOT[slot] % 4
        return acts.at[pl.ds(q * ROWS + half * HROWS + k * PIECE, PIECE)]

    def acts_sem(slot, half):
        if slot in NEAR:
            return a_recv.at[len(NEAR) if half else NEAR.index(slot)]
        return a_recv.at[len(NEAR) + 1 + next(i for i, slots in enumerate(TAKEN) if slot in slots)]

    def pass_on(slot, half, urgent):
        for sx, sy in steps_of(half, slot):
            there = ((slot[0] + sx) % NX, (slot[1] + sy) % NY)
            if urgent is None or (there in GROUPS[1]) == urgent:
                remote(
                    acts_rows(slot, half), acts_rows(there, half), acts_sem(there, half), in_plane(sx, sy)
                ).start()

    for half in range(2):
        pass_on((0, 0), half, None)

    def take_acts(slots, halves, urgent):
        arrived(acts.at[pl.ds(0, len(slots) * len(halves) * PIECE)], acts_sem(slots[0], halves[0]))
        for slot in slots:
            for half in halves:
                pass_on(slot, half, urgent)

    def multiply(q, strips):
        base, rows = strips[0] * HROWS, len(strips) * HROWS
        for cut in (pl.ds(0, FF), pl.ds(FF, FF)):
            part[q, base : base + rows, cut] = jnp.dot(
                acts[q * ROWS + base : q * ROWS + base + rows, :], w[:, cut], preferred_element_type=F32
            ).astype(BF16)
            for strip in strips:
                for d in range(2):
                    remote(
                        rows_of(q, strip, z_at(d, length(d, strip))).at[:, cut],
                        ring.at[q, strip, 0, d, :, cut],
                        r_recv.at[q, strip, 0],
                        along_z(toward(d)),
                    ).start()

    def toward(d):
        return 1 - 2 * d

    def z_at(d, hops):
        return (z + NZ + toward(d) * hops) % NZ

    def rows_of(q, strip, owner):
        return part.at[q, pl.ds(pl.multiple_of(strip * HROWS + owner * STRIP, STRIP), STRIP)]

    def received(q, strip, hop):
        ref = ring.at[q, strip, hop] if hop < HOPS - 1 else ring.at[q, strip, hop, strip]
        arrived(ref, r_recv.at[q, strip, hop])

    def piece(owner, q):
        return hidden.at[owner, pl.ds(q * PIECE, PIECE)]

    def gather_step(q, hop):
        if hop > 0:
            both = 2 * (PIECE if hop < HOPS else STRIP)
            arrived(hidden.at[0, pl.ds(0, both)], h_recv.at[q, hop - 1])
        if hop < HOPS:
            for d in range(2):
                goes = piece(z_at(d, -hop), q)
                if hop == HOPS - 1:
                    goes = hidden.at[z_at(d, -hop), pl.ds(q * PIECE + d * STRIP, STRIP)]
                remote(goes, goes, h_recv.at[q, hop], along_z(toward(d))).start()

    def ring_step(q, strip, stage):
        received(q, strip, stage - 1)
        for d in range(2):
            left = length(d, strip) - stage
            if left > 0:
                got = ring.at[q, strip, stage - 1, d]
                own = rows_of(q, strip, z_at(d, left))
                got[...] = (got[...].astype(F32) + own[...].astype(F32)).astype(BF16)
                remote(got, ring.at[q, strip, stage, d], r_recv.at[q, strip, stage], along_z(toward(d))).start()

    def finish(q):
        for strip in range(2):
            received(q, strip, HOPS - 1)
            a, b = ring.at[q, strip, HOPS - 1, strip], ring.at[q, strip, HOPS - 2, 1 - strip]
            own = rows_of(q, strip, z)
            gate, up = (
                a[:, cut].astype(F32) + b[:, cut].astype(F32) + own[:, cut].astype(F32)
                for cut in (pl.ds(0, FF), pl.ds(FF, FF))
            )
            value = gate / (1.0 + jnp.exp(-gate)) * up
            hidden[z, pl.ds(q * PIECE + strip * STRIP, STRIP), :] = value.astype(BF16)

    def lookup(q, k, axis):
        packed = sum(s[axis] * 4**i for i, s in enumerate(GROUPS[q]))
        return packed // ((1 + 3 * (k % 2)) * (1 + 15 * (k // 2))) % 4

    def down(q, hop):
        if hop == 0:
            turns = [(0, z)]
        elif hop < HOPS:
            turns = [(2 * hop - 1, (z + NZ - hop) % NZ), (2 * hop, (z + hop) % NZ)]
        else:
            turns = [(NZ - 1, (z + HOPS) % NZ)]
        from_rows = pl.ds(q * PIECE, PIECE)
        value = jnp.concatenate([hidden[owner, from_rows, :] for _, owner in turns], axis=0)

        def multiply_by(e):
            product = jnp.dot(value, wdt[e], preferred_element_type=F32).astype(BF16)
            for i, (turn, _) in enumerate(turns):
                outs[turn, e, from_rows, 0:D_ROW] = product[i * PIECE : (i + 1) * PIECE]

        def goes_to(turn, owner):
            k = owner // 2
            to_rows = pl.ds(pl.multiple_of(core * HALF + owner % 2 * PIECE, PIECE), PIECE)
            there = (y + NY - lookup(q, k, 1)) % NY * NX + (x + NX - lookup(q, k, 0)) % NX

            def send(to_core, sem=1 + q):
                remote(
                    outs.at[turn, to_core, from_rows],
                    finals.at[q * 4 + k, to_rows],
                    f_recv.at[sem],
                    (z * CORES + to_core, there),
                ).start()

            return k, to_rows, send

        for e in range(CORES):
            multiply_by(e)
        for turn, owner in turns:
            k, to_rows, send = goes_to(turn, owner)
            if q > 0:
                for e in range(CORES):
                    send(e)
                continue

            @pl.when(k == 0)
            def _():
                send(other, 0)
                finals[0, to_rows, :] = outs[turn, core, from_rows, :]

            @pl.when(k != 0)
            def _():
                send(other)
                send(core)

    def weights(which):
        ref = w.at[pl.ds(0, D_ROW)] if which == 0 else wd.at[0]
        pltpu.make_async_copy(ref, ref, w_local.at[which]).wait()
        arrived(ref, w_recv.at[which])
        if which == 1:
            for e in range(CORES):
                for tile in range(FF // 128):
                    cut = slice(tile * 128, (tile + 1) * 128)
                    wdt[e, cut, :] = wd[e, :, cut].astype(F32).T.astype(BF16)

    act = {
        "weights": weights, "take": take_acts, "pass_on": pass_on, "up": multiply, "ring": ring_step,
        "finish": finish, "gather": gather_step, "down": down,
    }
    for name, *at in order():
        act[name](*at)

    rest = finals.at[pl.ds(1, NX * NY - 1)]
    near = finals.at[0, pl.ds(pl.multiple_of(other * HALF, HALF), HALF)]
    for q in reversed(range(NQ)):
        first = 4 * q
        if q == 0:
            arrived(near, f_recv.at[0])
            arrived(finals.at[pl.ds(1, 3)], f_recv.at[1])
        else:
            arrived(finals.at[pl.ds(first, 4)], f_recv.at[1 + q])
        for tile in range(PAD // 128):
            cut = pl.ds(tile * 128, 128)
            value = finals[first, :, cut].astype(F32)
            for k in range(first + 1, first + 4):
                value = value + finals[k, :, cut].astype(F32)
            if q < NQ - 1:
                value = value + sums[:, cut]
            if q > 0:
                sums[:, cut] = value
                continue
            value = jnp.concatenate([value[STRIP * i : STRIP * (i + 1)] for i in (0, 2, 1, 3, 4, 6, 5, 7)], axis=0)
            rows = min(128, D_ROW - tile * 128)
            out_ref[tile * 128 : tile * 128 + rows, :] = value.T[0:rows, :].astype(out_ref.dtype)

    for ref in (
        swapped, w.at[pl.ds(0, D_ROW)], wd.at[0], acts.at[pl.ds(HALF, (NX * NY - 1) * HALF)],
        ring.at[pl.ds(0, NQ - 1)], ring.at[NQ - 1, 0], hidden.at[pl.ds(0, NZ - 1)], rest, near,
    ):
        remote(ref, ref, swap_recv, partner).wait_send()


def solution(mesh):
    def step(act_codes, act_scales, gate_weight, up_weight, down_weight):
        dma = pltpu.SemaphoreType.DMA
        return pl.pallas_call(
            kernel,
            out_shape=pltpu.VMEM((D_ROW, TOK), BF16),
            in_specs=[pl.BlockSpec(memory_space=pltpu.HBM)] * 5,
            out_specs=pl.BlockSpec(memory_space=pltpu.VMEM),
            scratch_shapes=[
                pltpu.VMEM((D_ROW, TOK), jnp.int32),
                pltpu.VMEM((7, TOK), F32),
                pltpu.VMEM((TOK, PAD), BF16),
                pltpu.VMEM((HALF, PAD), BF16),
                pltpu.VMEM((NX * NY * HALF, D_CHIP), BF16),
                pltpu.VMEM((D_CHIP, GU), BF16),
                pltpu.VMEM((CORES, D_ROW, FF), BF16),
                pltpu.VMEM((NQ, ROWS, GU), BF16),
                pltpu.VMEM((NQ, 2, HOPS, 2, STRIP, GU), BF16),
                pltpu.VMEM((NZ, NQ * PIECE, FF), BF16),
                pltpu.VMEM((NZ, CORES, NQ * PIECE, PAD), BF16),
                pltpu.VMEM((NX * NY, TOK, PAD), BF16),
                pltpu.VMEM((TOK, PAD), F32),
                pltpu.VMEM((CORES, FF, D_ROW), BF16),
                dma,
                dma((2,)),
                dma((2,)),
                dma((2,)),
                dma,
                dma((len(NEAR) + 1 + len(TAKEN),)),
                dma((NQ, 2, HOPS)),
                dma((NQ, HOPS)),
                dma((1 + NQ,)),
            ],
            compiler_params=pltpu.CompilerParams(
                collective_id=0, has_side_effects=True, vmem_limit_bytes=56_000_000
            ),
        )(*(
            pltpu.with_memory_space_constraint(array, pltpu.HBM)
            for array in (act_codes.T, act_scales.T, gate_weight, up_weight, down_weight.T)
        )).T

    return jax.shard_map(
        step,
        mesh=mesh,
        in_specs=(P("col", "row"), P("col", "row"), P("row", "col"), P("row", "col"), P("col", "row")),
        out_specs=P("col", "row"),
        check_vma=False,
    )
```
